32 devices in a mesh: row: 8 (over z, y), col: 4 (over x, core).
Axes of the slice: x: 2, y: 2, z: 4, core: 2. Of those that a mesh axis runs over, the one named last changes fastest.
Arguments:
- new_dosage: float32 [4096, 1024], P(('col', 'row')), may hold values from 0 to 2
- old_dosage: float32 [16384, 1024], P(('row', 'col')), may hold values from 0 to 2
- grm: bfloat16 [16384, 4096], P('row', 'col'), may hold values from -1.5 to 1.5
- counts: int32 [8], P('col'), may hold values from 256 to 512
- affected: int32 [32, 8], P('row', 'col'), may hold values from 0 to 1, as said below
Outputs:
- updated: bfloat16 [16384, 4096], P('row', 'col')
The draws below stay inside these ranges and needn't reach their ends.
Inputs may be any that keep to these rules, and one draw needn't show every extreme that they name: `affected`: the density of marked tile pairs differs from one tile of new samples to the next.
All inputs are finite; a program needn't handle non-finite values.
Results may differ from the reference program's by a relative error of at most 0.00115.
Values may be sent and summed in bfloat16 or wider, within the bound.
A program may use at most 128 MiB of HBM per device.

```python
import jax
import jax.numpy as jnp
from jax import lax

SNP = 1024
TILE = 512
REF_DEV = 2048
ALL = 16384
NEW = 4096
N_ROW = 8


def frequency_table(key):
    base_key, shift_key = jax.random.split(jax.random.fold_in(key, 5))
    base_rate = jax.random.uniform(base_key, (1, SNP), jnp.float32, 0.2, 0.8)
    shift_table = jax.random.uniform(shift_key, (16, SNP), jnp.float32, -0.15, 0.15)
    return base_rate + shift_table


def dosage_common(key, own_key, sample_count):
    frequency = frequency_table(key)
    subkeys = jax.random.split(own_key, 4)
    population = jax.random.randint(subkeys[0], (sample_count,), 0, 16)
    jitter = jax.random.uniform(subkeys[1], (sample_count, 1), jnp.float32, -0.02, 0.02)
    chance = jnp.clip(frequency[population] + jitter, 0.03, 0.97)
    allele_draw = jax.random.uniform(subkeys[2], (sample_count, SNP), jnp.float32, 0.0, 1.0)
    absent = (1.0 - chance) * (1.0 - chance)
    called = (allele_draw > absent).astype(jnp.float32) + (allele_draw > 1.0 - chance * chance).astype(jnp.float32)
    weight_draw = jax.random.uniform(subkeys[3], (sample_count, SNP), jnp.float32, 0.0, 1.0)
    shrinkage = 0.3 * weight_draw
    dosage = (1.0 - shrinkage) * called + shrinkage * 2.0 * chance
    return jnp.clip(dosage, 0.0, 2.0).astype(jnp.float32)


def draw_new_dosage(key, part):
    return dosage_common(key, jax.random.fold_in(key, 11), NEW)


def draw_old_dosage(key, part):
    return dosage_common(key, jax.random.fold_in(key, 23), ALL)


def draw_affected(key, part):
    first_key, second_key = jax.random.split(jax.random.fold_in(key, 37))
    offset = jax.random.randint(first_key, (), 0, 4)
    density = 1 + (jnp.arange(NEW // TILE) + offset) % 4
    tickets = jax.random.randint(second_key, (ALL // TILE, NEW // TILE), 0, 4)
    return (tickets < density[None, :]).astype(jnp.int32)


def touch_ends(drawn, key, least, top_value):
    dims = drawn.shape
    place = [jax.random.randint(jax.random.fold_in(key, axis), (), 0, dims[axis]) for axis in range(len(dims))]
    drawn = drawn.at[tuple(place)].set(least)
    longest = dims.index(max(dims))
    place[longest] = (place[longest] + 1) % dims[longest]
    return drawn.at[tuple(place)].set(top_value)


def level_of(key, shape, pieces, low, high):
    factor_of = 1.0
    for position, shards_of in pieces:
        draws = jax.random.uniform(jax.random.fold_in(jax.random.fold_in(key, 6), position), (shards_of,), jnp.float32, low / len(pieces), high / len(pieces))
        factor_of = factor_of * jnp.repeat(jnp.exp(draws), shape[position] // shards_of).reshape((-1,) + (1,) * (len(shape) - 1 - position))
    return factor_of


def gaussian(rng, shape, width, bound, cuts=(), held_as=jnp.bfloat16):
    values = width * jax.random.normal(rng, shape, jnp.float32)
    if cuts:
        values = values * level_of(rng, shape, cuts, -0.22, 0.18)
    return jnp.clip(values, -bound, bound).astype(held_as)


def setup_inputs(seed: int = 0) -> dict:
    arg_keys = jax.random.split(jax.random.key(seed), 6)
    new_dosage = draw_new_dosage(jax.random.fold_in(arg_keys[5], 71), 0)
    old_dosage = draw_old_dosage(jax.random.fold_in(arg_keys[5], 71), 0)
    grm = gaussian(arg_keys[2], (ALL, NEW), 0.1, 1.5, ((0, 8), (1, 4)))
    counts = touch_ends(jax.random.randint(arg_keys[3], (NEW // TILE,), TILE // 2, TILE + 1), jax.random.fold_in(arg_keys[3], 1), TILE // 2, TILE).astype(jnp.int32)
    affected = draw_affected(jax.random.fold_in(arg_keys[5], 71), 0)
    return {"new_dosage": new_dosage, "old_dosage": old_dosage, "grm": grm, "counts": counts, "affected": affected}


def reference(new_dosage, old_dosage, grm, counts, affected):
    totals = lax.optimization_barrier(jnp.sum(old_dosage, axis=0))
    doubled = totals / ALL
    spread = jnp.sqrt(doubled * (1.0 - 0.5 * doubled) + 0.1)
    usable = (jnp.arange(TILE)[None, :] < counts[:, None]).reshape(NEW).astype(jnp.float32)
    new_scores = ((new_dosage - doubled) / spread * usable[:, None]).astype(jnp.bfloat16)
    old_scores = ((old_dosage - doubled) / spread).astype(jnp.bfloat16)
    new_wide = new_scores.astype(jnp.float32)
    old_blocks = old_scores.reshape(N_ROW, REF_DEV, SNP)
    grm_blocks = grm.reshape(N_ROW, REF_DEV, NEW)
    mark_blocks = affected.reshape(N_ROW, REF_DEV // TILE, NEW // TILE)

    def update_block(operands):
        scores, grm_block, markers = operands
        product = jnp.dot(scores.astype(jnp.float32), new_wide.T, precision=lax.Precision.HIGHEST) / SNP
        spread_marks = jnp.repeat(jnp.repeat(markers.astype(jnp.float32), TILE, axis=0), TILE, axis=1)
        return (grm_block.astype(jnp.float32) + product * spread_marks).astype(jnp.bfloat16)
    updated = lax.map(update_block, (old_blocks, grm_blocks, mark_blocks))
    return updated.reshape(ALL, NEW)
```

```python
import functools

import jax
import jax.numpy as jnp
from jax import lax
from jax.experimental import pallas as pl
from jax.experimental.pallas import tpu as pltpu
from jax.sharding import PartitionSpec as P

MESH = pl.DeviceIdType.MESH
CORES = 2
SPLIT = (4, 4, 4, 2, 2)
CODED = 3
NEW_CHUNKS = 2
FOLD = 128
LEVELS = 32767
STRIP = 32


def sizes_of(n_row, n_col, new_rows, old_rows):
    minor = 1 << ((n_row.bit_length() - 1) // 2)
    whole = sum(SPLIT)
    offs = [old_rows * sum(SPLIT[:k]) // whole for k in range(len(SPLIT) + 1)]
    return minor, n_row // minor, n_col // CORES, offs


def ds(start, size, step):
    return pl.ds(pl.multiple_of(start, step), size)


def slot_place(a, major, t):
    near = jnp.minimum(a, major - 1 - a)
    step = (t + 1) // 2
    both = a - step if t % 2 else a + step
    left = a - (t - near)
    right = a + (t - near)
    one = jnp.where(a > major - 1 - a, left, right)
    return jnp.where(t <= 2 * near, both, one) if t else a


def kernel(
    n_row, n_col, new_hbm, old_hbm, grm_hbm, counts_hbm, affected_hbm,
    res, old_buf, new_buf, gain,
    new_in, old_in, new_code, old_code, part, part_y, part_z, counts, affected,
    load_sem, sum_recv, far, x_recv, sib_recv, own_recv, new_recv, sent,
):
    snps = new_in.shape[1]
    new_rows, old_rows = new_in.shape[0], old_in.shape[0]
    out_rows, out_cols = res.shape
    tile = out_cols // counts.shape[0]
    minor, major, chips, offs = sizes_of(n_row, n_col, new_rows, old_rows)
    pieces = len(offs) - 1
    last = pieces - 1
    new_chunk = new_rows // NEW_CHUNKS
    final = NEW_CHUNKS - 1
    group = minor * new_rows
    folds = snps // FOLD
    unit = new_chunk

    row, col = lax.axis_index("row"), lax.axis_index("col")
    a, b = row // minor, row % minor
    chip, core = col // CORES, col % CORES
    sibling = chip * CORES + (CORES - 1 - core)
    has_left, has_right = a > 0, a < major - 1

    def span(k):
        return offs[k + 1] - offs[k]

    grain = min(span(k) for k in range(pieces))

    cut = offs[1]
    old_loads = [
        pltpu.make_async_copy(
            old_hbm.at[pl.ds(lo, hi - lo), :], old_in.at[pl.ds(lo, hi - lo), :], load_sem.at[i]
        )
        for i, (lo, hi) in enumerate(((0, cut), (cut, old_rows)))
    ]
    new_load = pltpu.make_async_copy(new_hbm, new_in, load_sem.at[2])
    grm_load = pltpu.make_async_copy(grm_hbm, res, load_sem.at[3])
    counts_load = pltpu.make_async_copy(counts_hbm, counts, load_sem.at[4])
    affected_load = pltpu.make_async_copy(affected_hbm, affected, load_sem.at[5])
    old_loads[0].start()
    new_load.start()
    for load in old_loads[1:]:
        load.start()
    counts_load.start()
    affected_load.start()

    barrier = pltpu.get_barrier_semaphore()

    def greet(device):
        pl.semaphore_signal(barrier, inc=1, device_id=device, device_id_type=MESH)

    for d in range(1, n_col):
        greet((row, (col + d) % n_col))
    for d in range(1, minor):
        greet((a * minor + (b + d) % minor, col))

    @pl.when(has_left)
    def _():
        greet((row - minor, col))

    @pl.when(has_right)
    def _():
        greet((row + minor, col))

    def score_place(j, k):
        return j // CORES * (CORES * old_rows) + CORES * offs[k] + j % CORES * span(k)

    def code_place(j, k):
        return j // CORES * (CORES * offs[CODED]) + CORES * offs[k] + j % CORES * span(k)

    def exact_part(j, k):
        return old_buf.at[ds(score_place(j, k), span(k), grain), :]

    def old_part(j, k):
        if k < CODED:
            return old_code.at[ds(code_place(j, k), span(k), grain), :]
        return exact_part(j, k)

    own_start = col * old_rows

    def own_part(k):
        if k < CODED:
            return old_part(col, k)
        return old_buf.at[ds(own_start + offs[k], span(k), grain), :]

    def new_part(r, k):
        return new_code.at[ds(r * new_rows + k * new_chunk, new_chunk, new_chunk), :]

    def far_copy(k, d):
        return pltpu.make_async_remote_copy(
            own_part(k), old_part(col, k), sent.at[0], x_recv.at[chips - d - 1, k],
            device_id=(row, (chip + d) % chips * CORES + core), device_id_type=MESH,
        )

    def far_taken(k, d):
        j = (chip + d) % chips * CORES + core
        return pltpu.make_async_remote_copy(
            old_part(j, k), old_part(j, k), sent.at[0], x_recv.at[d - 1, k],
            device_id=(row, j), device_id_type=MESH,
        )

    def pass_copy(k, d, which):
        j = (chip + d) % chips * CORES + which
        return pltpu.make_async_remote_copy(
            old_part(j, k), old_part(j, k), sent.at[0], sib_recv.at[d - 1, k],
            device_id=(row, sibling), device_id_type=MESH,
        )

    def own_copy(j):
        part_of = old_buf.at[ds(j * old_rows, old_rows, grain), :]
        return pltpu.make_async_remote_copy(
            part_of, part_of, sent.at[0], own_recv.at[0],
            device_id=(row, sibling), device_id_type=MESH,
        )

    def new_copy(r, k, to):
        return pltpu.make_async_remote_copy(
            new_part(r, k), new_part(r, k), sent.at[0], new_recv.at[r, k],
            device_id=(to, col), device_id_type=MESH,
        )

    sends = []

    def start(copy, cond=None):
        if cond is None:
            copy.start()
        else:
            @pl.when(cond)
            def _():
                copy.start()
        sends.append((cond, copy))

    def is_end(z):
        return (z == 0) | (z == major - 1)

    def encode(x):
        return ((x * LEVELS + 0.5).astype(jnp.int32) - LEVELS).astype(jnp.int16)

    def encode_old(k):
        old_code[ds(code_place(col, k), span(k), grain), :] = encode(
            old_in[offs[k]:offs[k + 1], :]
        )

    with jax.named_scope("load"):
        old_loads[0].wait()
        encode_old(0)
        new_load.wait()
        new_code[ds(row * new_rows, new_rows, new_rows), :] = encode(new_in[...])
        for load in old_loads[1:]:
            load.wait()
        grm_load.start()
        mine = jnp.sum(old_in[...], axis=0, keepdims=True)
        for f in range(folds):
            part[pl.ds(col, 1), f, :] = mine[:, f * FOLD:(f + 1) * FOLD]

    def send_sums(buf, me, count, recv, target):
        for d in range(1, count):
            copy = pltpu.make_async_remote_copy(
                buf.at[me], buf.at[me], sent.at[0], recv,
                device_id=target((me + d) % count), device_id_type=MESH,
            )
            start(copy)

    def take_sums(buf, me, count, recv, target):
        rest = buf.at[pl.ds(0, count - 1)]
        pltpu.make_async_copy(rest, rest, recv).wait()
        total = buf[0]
        for i in range(1, count):
            total = total + buf[i]
        return total

    over_col = (part, col, n_col, sum_recv.at[0], lambda i: (row, i))
    over_mid = (part_y, b, minor, sum_recv.at[1], lambda i: (a * minor + i, col))
    over_row = (part_z, a, major, sum_recv.at[2], lambda i: (i * minor + b, col))

    def far_tell(h):
        @pl.when(has_right & (a - (h - 1) >= 0))
        def _():
            pl.semaphore_signal(
                far.at[h - 2], inc=1, device_id=(row + minor, col), device_id_type=MESH
            )

        @pl.when(has_left & (a + (h - 1) <= major - 1))
        def _():
            pl.semaphore_signal(
                far.at[h - 2], inc=1, device_id=(row - minor, col), device_id_type=MESH
            )

    def far_hear(h):
        heard = (a - h >= 0).astype(jnp.int32) + (a + h <= major - 1).astype(jnp.int32)

        @pl.when(heard > 0)
        def _():
            pl.semaphore_wait(far.at[h - 2], heard)

    def send_z(k):
        start(new_copy(row, k, row + minor), has_right)
        start(new_copy(row, k, row - minor), has_left)

    def send_y(z, k, cond=None):
        for d in range(1, minor):
            start(new_copy(z * minor + b, k, a * minor + (b + d) % minor), cond)

    def send_old(k):
        for d in range(1, chips):
            start(far_copy(k, d))

    with jax.named_scope("barrier"):
        pl.semaphore_wait(
            barrier,
            n_col - 1 + minor - 1 + has_left.astype(jnp.int32) + has_right.astype(jnp.int32),
        )
    with jax.named_scope("first"):
        send_sums(*over_col)
        send_old(0)
        send_z(0)
        send_y(a, 0)
        far_tell(2)
        for k in range(1, CODED):
            encode_old(k)
            send_old(k)
        for k in range(1, NEW_CHUNKS):
            send_z(k)
    with jax.named_scope("sumcol"):
        part_y[b] = take_sums(*over_col)
        send_sums(*over_mid)
        for k in range(1, NEW_CHUNKS):
            send_y(a, k)
        for h in range(2, major):
            far_hear(h)
            if h + 1 < major:
                far_tell(h + 1)
    with jax.named_scope("sumy"):
        part_z[a] = take_sums(*over_mid)
        send_sums(*over_row)


    def sided(s):
        for left in (True, False):
            z = a - 1 - s if left else a + 1 + s
            valid = z >= 0 if left else z < major
            onward = valid & (has_right if left else has_left)
            dest = row + minor if left else row - minor
            yield z, valid, onward, dest

    def relay(s, k):
        for z, valid, onward, dest in sided(s):
            r = z * minor + b

            @pl.when(valid)
            def _():
                new_copy(r, k, row).wait_recv()
            start(new_copy(r, k, dest), onward)
            across = valid & jnp.logical_not(is_end(z)) if k == final else valid
            send_y(z, k, across)

    def relay_first(s):
        for z, valid, onward, dest in sided(s):
            for d in range(1, minor):
                r = z * minor + (b + d) % minor

                @pl.when(valid & is_end(z))
                def _():
                    new_copy(r, final, row).wait_recv()
                start(new_copy(r, final, dest), onward & is_end(z))

    def own_first():
        for d in range(1, minor):
            r = a * minor + (b + d) % minor
            new_copy(r, final, row).wait_recv()
            start(new_copy(r, final, row + minor), a == 0)
            start(new_copy(r, final, row - minor), a == major - 1)

    def wait_y(t):
        z = slot_place(a, major, t)
        for k in range(NEW_CHUNKS):
            if t == 0 and k == final:
                continue
            for d in range(1, minor):
                r = z * minor + (b + d) % minor
                copy = new_copy(r, k, row)
                if k < final:
                    copy.wait_recv()
                else:
                    @pl.when(jnp.logical_not(is_end(z)))
                    def _():
                        copy.wait_recv()

    def forward_old(k):
        for d in range(1, chips):
            far_taken(k, d).wait_recv()
            start(pass_copy(k, d, core))

    def wait_sib_own():
        own_copy(sibling).wait_recv()

    def wait_sib_forwarded(k):
        for d in range(1, chips):
            pass_copy(k, d, CORES - 1 - core).wait_recv()

    def add(rows, z, product, row_tile):
        cols = ds(z * group, group, group)
        mark = affected[(z * group) // tile, row_tile].astype(jnp.float32)
        res[rows, cols] = (
            res[rows, cols].astype(jnp.float32) + product * (mark / snps)
        ).astype(jnp.bfloat16)

    def product_of(first, height, step, t0, tn):
        return lax.dot_general(
            old_buf[ds(first, height, step), :], new_buf[t0 * group:(t0 + tn) * group, :],
            (((1,), (1,)), ((), ())), preferred_element_type=jnp.float32,
        )

    def block(where, k0, k1, t0, tn):
        low = CORES * offs[k0]
        height = CORES * (offs[k1] - offs[k0])
        product = product_of(where * CORES * old_rows + low, height, grain, t0, tn)
        for i in range(tn):
            z = slot_place(a, major, t0 + i)
            for k in range(k0, k1):
                for c in range(CORES):
                    first = (where * CORES + c) * old_rows + offs[k]
                    at = CORES * offs[k] - low + c * span(k)
                    add(
                        ds(first, span(k), grain), z,
                        product[at:at + span(k), i * group:(i + 1) * group], first // tile,
                    )

    def local_rows(t0, tn):
        step = min(tile, CORES * old_rows)

        @pl.loop(0, CORES * old_rows // step)
        def _(i):
            first = chip * CORES * old_rows + i * step
            product = product_of(first, step, step, t0, tn)
            for j in range(tn):
                add(
                    ds(first, step, step), slot_place(a, major, t0 + j),
                    product[:, j * group:(j + 1) * group], first // tile,
                )

    def far_rows(k0, k1, t0, tn):
        for d in range(1, chips):
            block((chip + d) % chips, k0, k1, t0, tn)

    with jax.named_scope("relay0"):
        relay(0, 0)
    with jax.named_scope("relay1"):
        for k in range(1, NEW_CHUNKS):
            relay(0, k)
    with jax.named_scope("own_first"):
        own_first()
    with jax.named_scope("x0"):
        forward_old(0)
    with jax.named_scope("sumz"):
        total = take_sums(*over_row)
    totals = jnp.concatenate([total[f:f + 1] for f in range(folds)], axis=1)
    doubled = totals / (old_rows * n_row * n_col)
    inverse = 1.0 / jnp.sqrt(doubled * (1.0 - 0.5 * doubled) + 0.1)
    code_scale = inverse / LEVELS
    code_shift = (1.0 - doubled) * inverse

    def score(k):
        old_buf[ds(own_start + offs[k], span(k), grain), :] = (
            (old_in[offs[k]:offs[k + 1], :] - doubled) * inverse
        ).astype(jnp.bfloat16)

    with jax.named_scope("score"):
        for k in range(CODED, pieces):
            score(k)
            send_old(k)
        for k in range(CODED):
            score(k)
        start(own_copy(col))
        counts_load.wait()
        affected_load.wait()
        grm_load.wait()

    def decode(codes):
        return codes.astype(jnp.int32).astype(jnp.float32) * code_scale + code_shift

    def decode_new(t):
        z = slot_place(a, major, t)
        count = counts[(z * group) // tile]

        @pl.loop(0, group // STRIP)
        def _(i):
            at = z * group + i * STRIP
            place = lax.broadcasted_iota(jnp.int32, (STRIP, 1), 0) + at % tile
            usable = (place < count).astype(jnp.float32)
            codes = new_code[ds(at, STRIP, STRIP), :]
            new_buf[ds(t * group + i * STRIP, STRIP, STRIP), :] = (
                decode(codes) * usable
            ).astype(jnp.bfloat16)

    def decode_old(k):
        if k >= CODED:
            return
        strip = min(STRIP, CORES * span(k))
        for d in range(1, chips):
            j = (chip + d) % chips * CORES

            @pl.loop(0, CORES * span(k) // strip)
            def _(i):
                codes = old_code[ds(code_place(j, k) + i * strip, strip, strip), :]
                old_buf[ds(score_place(j, k) + i * strip, strip, strip), :] = (
                    decode(codes).astype(jnp.bfloat16)
                )

    def take_group(t):
        with jax.named_scope("wy%d" % t):
            wait_y(t)
        with jax.named_scope("dec%d" % t):
            decode_new(t)

    def take_old(k):
        with jax.named_scope("ws%d" % k):
            wait_sib_forwarded(k)
            decode_old(k)

    with jax.named_scope("gain"):
        for i in range(out_rows // tile):
            for j in range(out_cols // tile):
                mark = affected[j, i].astype(jnp.float32)
                gain[i:i + 1, j * tile:(j + 1) * tile] = jnp.full(
                    (1, tile), mark / snps, jnp.float32
                )

    def relayed(s, k):
        with jax.named_scope("relay%d_%d" % (s, k)):
            relay(s, k)

    def relayed_first(s):
        with jax.named_scope("first%d" % s):
            relay_first(s)

    def forwarded(k):
        with jax.named_scope("x%d" % k):
            forward_old(k)

    def local(t0, tn):
        with jax.named_scope("mm_local%d" % t0):
            local_rows(t0, tn)

    def distant(k0, k1, t0, tn):
        with jax.named_scope("mm_far%d_%d" % (k0, t0)):
            far_rows(k0, k1, t0, tn)

    half = major // 2
    take_group(0)
    for s in range(1, half):
        relayed(s, 0)
        relayed_first(s - 1)
        relayed(s, 1)
    forwarded(1)
    for t in range(1, half):
        take_group(t)
    with jax.named_scope("sibown"):
        wait_sib_own()
    local(0, half)
    take_old(0)
    take_old(1)
    distant(0, 2, 0, half)
    for s in range(half, major - 1):
        relayed(s, 0)
        relayed_first(s - 1)
        if s == half:
            forwarded(2)
        relayed(s, 1)
    for t in range(half, major - 1):
        take_group(t)
        local(t, 1)
        if t == half:
            take_old(2)
            distant(2, 3, 0, half)
        distant(0, 3, t, 1)
    forwarded(3)
    relayed_first(major - 2)
    take_group(major - 1)
    local(major - 1, 1)
    distant(0, 3, major - 1, 1)
    for k in range(3, pieces):
        take_old(k)
        if k + 1 < pieces:
            distant(k, k + 1, 0, major)
            forwarded(k + 1)

    with jax.named_scope("sends"):
        for cond, copy in sends:
            if cond is None:
                copy.wait_send()
            else:
                @pl.when(cond)
                def _():
                    copy.wait_send()


def finish(n_row, n_col, res, old_buf, new_buf, gain, out_hbm, stage, sem):
    out_rows, out_cols = res.shape
    old_rows, new_rows = out_rows // n_col, out_cols // n_row
    minor, major, chips, offs = sizes_of(n_row, n_col, new_rows, old_rows)
    group = minor * new_rows
    tile = out_rows // gain.shape[0]
    last = len(offs) - 2
    size = offs[last + 1] - offs[last]
    row, col = lax.axis_index("row"), lax.axis_index("col")
    a, chip = row // minor, col // CORES

    def out_copy(src, start, count, i):
        return pltpu.make_async_copy(src, out_hbm.at[ds(start, count, size), :], sem.at[i])

    copies = []
    mine = chip * CORES * old_rows
    copies.append(out_copy(res.at[ds(mine, CORES * old_rows, size), :], mine, CORES * old_rows, 0))
    places = []
    for d in range(1, chips):
        where = (chip + d) % chips
        for c in range(CORES):
            first = (where * CORES + c) * old_rows
            copies.append(out_copy(res.at[ds(first, offs[last], size), :], first, offs[last], len(copies)))
            places.append((d - 1, c, first + offs[last]))
    for copy in copies:
        copy.start()
    with jax.named_scope("tail"):
        for d in range(1, chips):
            where = (chip + d) % chips
            at = where * CORES * old_rows + CORES * offs[last]
            product = lax.dot_general(
                old_buf[ds(at, CORES * size, size), :], new_buf[...],
                (((1,), (1,)), ((), ())), preferred_element_type=jnp.float32,
            )
            for c in range(CORES):
                first = (where * CORES + c) * old_rows + offs[last]
                to = ((d - 1) * CORES + c) * size
                for t in range(major):
                    cols = ds(slot_place(a, major, t) * group, group, group)
                    stage[to:to + size, cols] = (
                        res[ds(first, size, size), cols].astype(jnp.float32)
                        + product[c * size:(c + 1) * size, t * group:(t + 1) * group]
                        * gain[pl.ds(first // tile, 1), cols]
                    ).astype(jnp.bfloat16)
                copy = out_copy(stage.at[pl.ds(to, size), :], first, size, len(copies))
                copy.start()
                copies.append(copy)
    for i, copy in enumerate(copies):
        with jax.named_scope('out%d' % i):
            copy.wait()


def on_device(new_dosage, old_dosage, grm, counts, affected):
    n_row, n_col = lax.axis_size("row"), lax.axis_size("col")
    new_rows, snps = new_dosage.shape
    old_rows = old_dosage.shape[0]
    out_rows, out_cols = grm.shape
    minor, major, chips, offs = sizes_of(n_row, n_col, new_rows, old_rows)
    pieces = len(offs) - 1
    dma = pltpu.SemaphoreType.DMA
    hbm = pl.BlockSpec(memory_space=pltpu.HBM)
    vmem = pl.BlockSpec(memory_space=pltpu.VMEM)
    row_tiles = affected.shape[0]
    res, old_buf, new_buf, gain = pl.pallas_call(
        functools.partial(kernel, n_row, n_col),
        out_shape=(
            pltpu.VMEM(grm.shape, grm.dtype),
            pltpu.VMEM((old_rows * n_col, snps), jnp.bfloat16),
            pltpu.VMEM((new_rows * n_row, snps), jnp.bfloat16),
            pltpu.VMEM((row_tiles, out_cols), jnp.float32),
        ),
        in_specs=[hbm] * 5,
        out_specs=(vmem,) * 4,
        scratch_shapes=[
            pltpu.VMEM((new_rows, snps), jnp.float32),
            pltpu.VMEM((old_rows, snps), jnp.float32),
            pltpu.VMEM((new_rows * n_row, snps), jnp.int16),
            pltpu.VMEM((offs[CODED] * n_col, snps), jnp.int16),
            pltpu.VMEM((n_col, snps // FOLD, FOLD), jnp.float32),
            pltpu.VMEM((minor, snps // FOLD, FOLD), jnp.float32),
            pltpu.VMEM((major, snps // FOLD, FOLD), jnp.float32),
            pltpu.SMEM(counts.shape, jnp.int32),
            pltpu.SMEM(affected.shape[::-1], jnp.int32),
            dma((6,)),
            dma((3,)),
            pltpu.SemaphoreType.REGULAR((max(1, major - 2),)),
            dma((chips - 1, pieces)),
            dma((chips - 1, pieces)),
            dma((1,)),
            dma((n_row, NEW_CHUNKS)),
            dma((1,)),
        ],
        compiler_params=pltpu.CompilerParams(
            collective_id=0, has_side_effects=True, vmem_limit_bytes=50 * 1024 * 1024
        ),
    )(new_dosage, old_dosage, grm, counts, affected.T)
    size = offs[-1] - offs[-2]
    return pl.pallas_call(
        functools.partial(finish, n_row, n_col),
        out_shape=jax.ShapeDtypeStruct(grm.shape, grm.dtype),
        in_specs=[vmem] * 4,
        out_specs=hbm,
        scratch_shapes=[
            pltpu.VMEM(((chips - 1) * CORES * size, out_cols), jnp.bfloat16),
            dma((1 + 2 * (chips - 1) * CORES,)),
        ],
        compiler_params=pltpu.CompilerParams(vmem_limit_bytes=12 * 1024 * 1024),
    )(res, old_buf, new_buf, gain)


def solution(mesh):
    return jax.shard_map(
        on_device,
        mesh=mesh,
        in_specs=(
            P(("col", "row"), None),
            P(("row", "col"), None),
            P("row", "col"),
            P("col"),
            P("row", "col"),
        ),
        out_specs=P("row", "col"),
        check_vma=False,
    )
```

```python
import functools

import jax
import jax.numpy as jnp
from jax import lax
from jax.experimental import pallas as pl
from jax.experimental.pallas import tpu as pltpu
from jax.sharding import PartitionSpec as P

MESH = pl.DeviceIdType.MESH
CORES = 2
SPLIT = (4, 4, 4, 2, 2)
CODED = 3
LATE = 3
NEW_CHUNKS = 2
FOLD = 128
LEVELS = 32767
STRIP = 32


def sizes_of(n_row, n_col, new_rows, old_rows):
    minor = 1 << ((n_row.bit_length() - 1) // 2)
    whole = sum(SPLIT)
    offs = [old_rows * sum(SPLIT[:k]) // whole for k in range(len(SPLIT) + 1)]
    return minor, n_row // minor, n_col // CORES, offs


def ds(start, size, step):
    return pl.ds(pl.multiple_of(start, step), size)


def slot_place(a, major, t):
    near = jnp.minimum(a, major - 1 - a)
    step = (t + 1) // 2
    both = a - step if t % 2 else a + step
    left = a - (t - near)
    right = a + (t - near)
    one = jnp.where(a > major - 1 - a, left, right)
    return jnp.where(t <= 2 * near, both, one) if t else a


def kernel(
    n_row, n_col, new_hbm, old_hbm, grm_hbm, counts_hbm, affected_hbm,
    res, old_buf, new_buf, gain,
    new_in, old_in, new_code, old_code, part, part_y, part_z, counts, affected,
    load_sem, sum_recv, far, x_recv, sib_recv, own_recv, new_recv, sent,
):
    snps = new_in.shape[1]
    new_rows, old_rows = new_in.shape[0], old_in.shape[0]
    out_rows, out_cols = res.shape
    tile = out_cols // counts.shape[0]
    minor, major, chips, offs = sizes_of(n_row, n_col, new_rows, old_rows)
    pieces = len(offs) - 1
    new_chunk = new_rows // NEW_CHUNKS
    final = NEW_CHUNKS - 1
    group = minor * new_rows
    folds = snps // FOLD
    unit = new_chunk

    row, col = lax.axis_index("row"), lax.axis_index("col")
    a, b = row // minor, row % minor
    chip, core = col // CORES, col % CORES
    sibling = chip * CORES + (CORES - 1 - core)
    has_left, has_right = a > 0, a < major - 1

    def span(k):
        return offs[k + 1] - offs[k]

    grain = min(span(k) for k in range(pieces))

    cut = offs[1]
    old_loads = [
        pltpu.make_async_copy(
            old_hbm.at[pl.ds(lo, hi - lo), :], old_in.at[pl.ds(lo, hi - lo), :], load_sem.at[i]
        )
        for i, (lo, hi) in enumerate(((0, cut), (cut, old_rows)))
    ]
    new_load = pltpu.make_async_copy(new_hbm, new_in, load_sem.at[2])
    grm_load = pltpu.make_async_copy(grm_hbm, res, load_sem.at[3])
    counts_load = pltpu.make_async_copy(counts_hbm, counts, load_sem.at[4])
    affected_load = pltpu.make_async_copy(affected_hbm, affected, load_sem.at[5])
    for load in old_loads:
        load.start()
    new_load.start()
    counts_load.start()
    affected_load.start()

    barrier = pltpu.get_barrier_semaphore()

    def greet(device):
        pl.semaphore_signal(barrier, inc=1, device_id=device, device_id_type=MESH)

    for d in range(1, n_col):
        greet((row, (col + d) % n_col))
    for d in range(1, minor):
        greet((a * minor + (b + d) % minor, col))

    @pl.when(has_left)
    def _():
        greet((row - minor, col))

    @pl.when(has_right)
    def _():
        greet((row + minor, col))

    def score_place(j, k):
        return j // CORES * (CORES * old_rows) + CORES * offs[k] + j % CORES * span(k)

    def code_place(j, k):
        return j // CORES * (CORES * offs[CODED]) + CORES * offs[k] + j % CORES * span(k)

    def exact_part(j, k):
        return old_buf.at[ds(score_place(j, k), span(k), grain), :]

    def old_part(j, k):
        if k < CODED:
            return old_code.at[ds(code_place(j, k), span(k), grain), :]
        return exact_part(j, k)

    own_start = col * old_rows

    def own_part(k):
        if k < CODED:
            return old_part(col, k)
        return old_buf.at[ds(own_start + offs[k], span(k), grain), :]

    def new_part(r, k):
        return new_code.at[ds(r * new_rows + k * new_chunk, new_chunk, new_chunk), :]

    def far_copy(k, d):
        return pltpu.make_async_remote_copy(
            own_part(k), old_part(col, k), sent.at[0], x_recv.at[chips - d - 1, k],
            device_id=(row, (chip + d) % chips * CORES + core), device_id_type=MESH,
        )

    def far_taken(k, d):
        j = (chip + d) % chips * CORES + core
        return pltpu.make_async_remote_copy(
            old_part(j, k), old_part(j, k), sent.at[0], x_recv.at[d - 1, k],
            device_id=(row, j), device_id_type=MESH,
        )

    def pass_copy(k, d, which):
        j = (chip + d) % chips * CORES + which
        return pltpu.make_async_remote_copy(
            old_part(j, k), old_part(j, k), sent.at[0], sib_recv.at[d - 1, k],
            device_id=(row, sibling), device_id_type=MESH,
        )

    def own_copy(j):
        part_of = old_buf.at[ds(j * old_rows, old_rows, grain), :]
        return pltpu.make_async_remote_copy(
            part_of, part_of, sent.at[0], own_recv.at[0],
            device_id=(row, sibling), device_id_type=MESH,
        )

    def new_copy(r, k, to):
        return pltpu.make_async_remote_copy(
            new_part(r, k), new_part(r, k), sent.at[0], new_recv.at[r, k],
            device_id=(to, col), device_id_type=MESH,
        )

    sends = []

    def start(copy, cond=None):
        if cond is None:
            copy.start()
        else:
            @pl.when(cond)
            def _():
                copy.start()
        sends.append((cond, copy))

    def is_end(z):
        return (z == 0) | (z == major - 1)

    def encode(x):
        return ((x * LEVELS + 0.5).astype(jnp.int32) - LEVELS).astype(jnp.int16)

    def encode_old(k):
        old_code[ds(code_place(col, k), span(k), grain), :] = encode(
            old_in[offs[k]:offs[k + 1], :]
        )

    def send_sums(buf, me, count, recv, target):
        for d in range(1, count):
            copy = pltpu.make_async_remote_copy(
                buf.at[me], buf.at[me], sent.at[0], recv,
                device_id=target((me + d) % count), device_id_type=MESH,
            )
            start(copy)

    def take_sums(buf, me, count, recv, target):
        rest = buf.at[pl.ds(0, count - 1)]
        pltpu.make_async_copy(rest, rest, recv).wait()
        total = buf[0]
        for i in range(1, count):
            total = total + buf[i]
        return total

    over_col = (part, col, n_col, sum_recv.at[0], lambda i: (row, i))
    over_mid = (part_y, b, minor, sum_recv.at[1], lambda i: (a * minor + i, col))
    over_row = (part_z, a, major, sum_recv.at[2], lambda i: (i * minor + b, col))

    def far_tell(h):
        @pl.when(has_right & (a - (h - 1) >= 0))
        def _():
            pl.semaphore_signal(
                far.at[h - 2], inc=1, device_id=(row + minor, col), device_id_type=MESH
            )

        @pl.when(has_left & (a + (h - 1) <= major - 1))
        def _():
            pl.semaphore_signal(
                far.at[h - 2], inc=1, device_id=(row - minor, col), device_id_type=MESH
            )

    def far_hear(h):
        heard = (a - h >= 0).astype(jnp.int32) + (a + h <= major - 1).astype(jnp.int32)

        @pl.when(heard > 0)
        def _():
            pl.semaphore_wait(far.at[h - 2], heard)

    def send_z(k):
        start(new_copy(row, k, row + minor), has_right)
        start(new_copy(row, k, row - minor), has_left)

    def send_y(z, k, cond=None):
        for d in range(1, minor):
            start(new_copy(z * minor + b, k, a * minor + (b + d) % minor), cond)

    def send_old(k):
        for d in range(1, chips):
            start(far_copy(k, d))

    with jax.named_scope("loadold"):
        old_loads[0].wait()
        encode_old(0)
        old_loads[1].wait()
        mine = jnp.sum(old_in[...], axis=0, keepdims=True)
        for f in range(folds):
            part[pl.ds(col, 1), f, :] = mine[:, f * FOLD:(f + 1) * FOLD]
    with jax.named_scope("barrier"):
        pl.semaphore_wait(
            barrier,
            n_col - 1 + minor - 1 + has_left.astype(jnp.int32) + has_right.astype(jnp.int32),
        )
    send_sums(*over_col)
    send_old(0)
    far_tell(2)
    with jax.named_scope("first"):
        new_load.wait()
        new_code[ds(row * new_rows, new_rows, new_rows), :] = encode(new_in[...])
        send_z(0)
        send_y(a, 0)
        grm_load.start()
        for k in range(1, CODED):
            encode_old(k)
            send_old(k)
        for k in range(1, NEW_CHUNKS):
            send_z(k)
    with jax.named_scope("sumcol"):
        part_y[b] = take_sums(*over_col)
        send_sums(*over_mid)
        for k in range(1, NEW_CHUNKS):
            send_y(a, k)
    with jax.named_scope("hear"):
        for h in range(2, major):
            far_hear(h)
            if h + 1 < major:
                far_tell(h + 1)
    with jax.named_scope("sumy"):
        part_z[a] = take_sums(*over_mid)
        send_sums(*over_row)


    def sided(s):
        for left in (True, False):
            z = a - 1 - s if left else a + 1 + s
            valid = z >= 0 if left else z < major
            onward = valid & (has_right if left else has_left)
            dest = row + minor if left else row - minor
            yield z, valid, onward, dest

    def relay(s, k):
        for z, valid, onward, dest in sided(s):
            r = z * minor + b

            @pl.when(valid)
            def _():
                new_copy(r, k, row).wait_recv()
            start(new_copy(r, k, dest), onward)
            across = valid & jnp.logical_not(is_end(z)) if k == final else valid
            send_y(z, k, across)

    def relay_first(s):
        for z, valid, onward, dest in sided(s):
            for d in range(1, minor):
                r = z * minor + (b + d) % minor

                @pl.when(valid & is_end(z))
                def _():
                    new_copy(r, final, row).wait_recv()
                start(new_copy(r, final, dest), onward & is_end(z))

    def own_first():
        for d in range(1, minor):
            r = a * minor + (b + d) % minor
            new_copy(r, final, row).wait_recv()
            start(new_copy(r, final, row + minor), a == 0)
            start(new_copy(r, final, row - minor), a == major - 1)

    def wait_y(t):
        z = slot_place(a, major, t)
        for k in range(NEW_CHUNKS):
            if t == 0 and k == final:
                continue
            for d in range(1, minor):
                r = z * minor + (b + d) % minor
                copy = new_copy(r, k, row)
                if k < final:
                    copy.wait_recv()
                else:
                    @pl.when(jnp.logical_not(is_end(z)))
                    def _():
                        copy.wait_recv()

    def forward_old(k):
        for d in range(1, chips):
            far_taken(k, d).wait_recv()
            start(pass_copy(k, d, core))

    def wait_sib_own():
        own_copy(sibling).wait_recv()

    def wait_sib_forwarded(k):
        for d in range(1, chips):
            pass_copy(k, d, CORES - 1 - core).wait_recv()

    def add(rows, z, product, row_tile):
        cols = ds(z * group, group, group)
        mark = affected[(z * group) // tile, row_tile].astype(jnp.float32)
        res[rows, cols] = (
            res[rows, cols].astype(jnp.float32) + product * (mark / snps)
        ).astype(jnp.bfloat16)

    def product_of(first, height, step, t0, tn):
        return lax.dot_general(
            old_buf[ds(first, height, step), :], new_buf[t0 * group:(t0 + tn) * group, :],
            (((1,), (1,)), ((), ())), preferred_element_type=jnp.float32,
        )

    def block(where, k0, k1, t0, tn):
        low = CORES * offs[k0]
        height = CORES * (offs[k1] - offs[k0])
        product = product_of(where * CORES * old_rows + low, height, grain, t0, tn)
        for i in range(tn):
            z = slot_place(a, major, t0 + i)
            for k in range(k0, k1):
                for c in range(CORES):
                    first = (where * CORES + c) * old_rows + offs[k]
                    at = CORES * offs[k] - low + c * span(k)
                    add(
                        ds(first, span(k), grain), z,
                        product[at:at + span(k), i * group:(i + 1) * group], first // tile,
                    )

    def local_rows(t0, tn):
        step = min(tile, CORES * old_rows)

        @pl.loop(0, CORES * old_rows // step)
        def _(i):
            first = chip * CORES * old_rows + i * step
            product = product_of(first, step, step, t0, tn)
            for j in range(tn):
                add(
                    ds(first, step, step), slot_place(a, major, t0 + j),
                    product[:, j * group:(j + 1) * group], first // tile,
                )

    def far_rows(k0, k1, t0, tn):
        for d in range(1, chips):
            block((chip + d) % chips, k0, k1, t0, tn)

    with jax.named_scope("relay0"):
        relay(0, 0)
    with jax.named_scope("relay1"):
        for k in range(1, NEW_CHUNKS):
            relay(0, k)
    with jax.named_scope("own_first"):
        own_first()
    with jax.named_scope("x0"):
        forward_old(0)
    with jax.named_scope("sumz"):
        total = take_sums(*over_row)
    totals = jnp.concatenate([total[f:f + 1] for f in range(folds)], axis=1)
    doubled = totals / (old_rows * n_row * n_col)
    inverse = 1.0 / jnp.sqrt(doubled * (1.0 - 0.5 * doubled) + 0.1)
    code_scale = inverse / LEVELS
    code_shift = (1.0 - doubled) * inverse

    def score(k):
        old_buf[ds(own_start + offs[k], span(k), grain), :] = (
            (old_in[offs[k]:offs[k + 1], :] - doubled) * inverse
        ).astype(jnp.bfloat16)

    with jax.named_scope("score"):
        for k in range(CODED, pieces):
            score(k)
            send_old(k)
        for k in range(CODED):
            score(k)
        start(own_copy(col))
        counts_load.wait()
        affected_load.wait()
        grm_load.wait()

    def decode(codes):
        return codes.astype(jnp.int32).astype(jnp.float32) * code_scale + code_shift

    def decode_new(t):
        z = slot_place(a, major, t)
        count = counts[(z * group) // tile]

        @pl.loop(0, group // STRIP)
        def _(i):
            at = z * group + i * STRIP
            place = lax.broadcasted_iota(jnp.int32, (STRIP, 1), 0) + at % tile
            usable = (place < count).astype(jnp.float32)
            codes = new_code[ds(at, STRIP, STRIP), :]
            new_buf[ds(t * group + i * STRIP, STRIP, STRIP), :] = (
                decode(codes) * usable
            ).astype(jnp.bfloat16)

    def decode_old(k):
        if k >= CODED:
            return
        strip = min(STRIP, CORES * span(k))
        for d in range(1, chips):
            j = (chip + d) % chips * CORES

            @pl.loop(0, CORES * span(k) // strip)
            def _(i):
                codes = old_code[ds(code_place(j, k) + i * strip, strip, strip), :]
                old_buf[ds(score_place(j, k) + i * strip, strip, strip), :] = (
                    decode(codes).astype(jnp.bfloat16)
                )

    def take_group(t):
        with jax.named_scope("wy%d" % t):
            wait_y(t)
        with jax.named_scope("dec%d" % t):
            decode_new(t)

    def take_old(k):
        with jax.named_scope("ws%d" % k):
            wait_sib_forwarded(k)
            decode_old(k)

    with jax.named_scope("gain"):
        for i in range(out_rows // tile):
            for j in range(out_cols // tile):
                mark = affected[j, i].astype(jnp.float32)
                gain[i:i + 1, j * tile:(j + 1) * tile] = jnp.full(
                    (1, tile), mark / snps, jnp.float32
                )

    def relayed(s, k):
        with jax.named_scope("relay%d_%d" % (s, k)):
            relay(s, k)

    def relayed_first(s):
        with jax.named_scope("first%d" % s):
            relay_first(s)

    def forwarded(k):
        with jax.named_scope("x%d" % k):
            forward_old(k)

    def local(t0, tn):
        with jax.named_scope("mm_local%d" % t0):
            local_rows(t0, tn)

    def distant(k0, k1, t0, tn):
        with jax.named_scope("mm_far%d_%d" % (k0, t0)):
            far_rows(k0, k1, t0, tn)

    half = major // 2
    take_group(0)
    for s in range(1, half):
        relayed(s, 0)
        relayed_first(s - 1)
        relayed(s, 1)
    forwarded(1)
    for t in range(1, half):
        take_group(t)
    with jax.named_scope("sibown"):
        wait_sib_own()
    local(0, half)
    for k in range(2):
        take_old(k)
    distant(0, 2, 0, half)
    for s in range(half, major - 1):
        relayed(s, 0)
        relayed_first(s - 1)
        if s == half:
            forwarded(2)
        relayed(s, 1)
    for t in range(half, major - 1):
        take_group(t)
        local(t, 1)
        distant(0, 2, t, 1)
    take_old(2)
    distant(2, LATE, 0, major - 1)
    forwarded(3)
    relayed_first(major - 2)
    take_group(major - 1)
    local(major - 1, 1)
    distant(0, LATE, major - 1, 1)
    for k in range(4, pieces):
        forwarded(k)
    for k in range(LATE, pieces):
        take_old(k)

    with jax.named_scope("sends"):
        for cond, copy in sends:
            if cond is None:
                copy.wait_send()
            else:
                @pl.when(cond)
                def _():
                    copy.wait_send()


def finish(n_row, n_col, res, old_buf, new_buf, gain, out_hbm, stage, sem):
    out_rows, out_cols = res.shape
    old_rows, new_rows = out_rows // n_col, out_cols // n_row
    minor, major, chips, offs = sizes_of(n_row, n_col, new_rows, old_rows)
    group = minor * new_rows
    tile = out_rows // gain.shape[0]
    early, size = offs[LATE], old_rows - offs[LATE]
    grain = min(hi - lo for lo, hi in zip(offs[:-1], offs[1:], strict=True))
    row, col = lax.axis_index("row"), lax.axis_index("col")
    a, chip = row // minor, col // CORES

    def out_copy(src, start, count):
        return pltpu.make_async_copy(
            src, out_hbm.at[ds(start, count, grain), :], sem.at[0]
        )

    mine = chip * CORES * old_rows
    copies = [
        out_copy(res.at[ds(mine, CORES * old_rows, grain), :], mine, CORES * old_rows)
    ]
    for d in range(1, chips):
        for c in range(CORES):
            first = ((chip + d) % chips * CORES + c) * old_rows
            copies.append(out_copy(res.at[ds(first, early, grain), :], first, early))
    for copy in copies:
        copy.start()
    with jax.named_scope("tail"):
        for d in range(1, chips):
            where = (chip + d) % chips
            low = where * CORES * old_rows + CORES * early
            product = lax.dot_general(
                old_buf[ds(low, CORES * size, grain), :], new_buf[...],
                (((1,), (1,)), ((), ())), preferred_element_type=jnp.float32,
            )
            for c in range(CORES):
                start_row = (where * CORES + c) * old_rows + early
                to = ((d - 1) * CORES + c) * size
                for k in range(LATE, len(offs) - 1):
                    span = offs[k + 1] - offs[k]
                    at = CORES * (offs[k] - early) + c * span
                    lead = offs[k] - early
                    first = start_row + lead
                    for t in range(major):
                        cols = ds(slot_place(a, major, t) * group, group, group)
                        stage[to + lead:to + lead + span, cols] = (
                            res[ds(first, span, grain), cols].astype(jnp.float32)
                            + product[at:at + span, t * group:(t + 1) * group]
                            * gain[pl.ds(first // tile, 1), cols]
                        ).astype(jnp.bfloat16)
                copy = out_copy(stage.at[pl.ds(to, size), :], start_row, size)
                copy.start()
                copies.append(copy)
    with jax.named_scope("out"):
        for copy in copies:
            copy.wait()


def on_device(new_dosage, old_dosage, grm, counts, affected):
    n_row, n_col = lax.axis_size("row"), lax.axis_size("col")
    new_rows, snps = new_dosage.shape
    old_rows = old_dosage.shape[0]
    out_rows, out_cols = grm.shape
    minor, major, chips, offs = sizes_of(n_row, n_col, new_rows, old_rows)
    pieces = len(offs) - 1
    dma = pltpu.SemaphoreType.DMA
    hbm = pl.BlockSpec(memory_space=pltpu.HBM)
    vmem = pl.BlockSpec(memory_space=pltpu.VMEM)
    row_tiles = affected.shape[0]
    res, old_buf, new_buf, gain = pl.pallas_call(
        functools.partial(kernel, n_row, n_col),
        out_shape=(
            pltpu.VMEM(grm.shape, grm.dtype),
            pltpu.VMEM((old_rows * n_col, snps), jnp.bfloat16),
            pltpu.VMEM((new_rows * n_row, snps), jnp.bfloat16),
            pltpu.VMEM((row_tiles, out_cols), jnp.float32),
        ),
        in_specs=[hbm] * 5,
        out_specs=(vmem,) * 4,
        scratch_shapes=[
            pltpu.VMEM((new_rows, snps), jnp.float32),
            pltpu.VMEM((old_rows, snps), jnp.float32),
            pltpu.VMEM((new_rows * n_row, snps), jnp.int16),
            pltpu.VMEM((offs[CODED] * n_col, snps), jnp.int16),
            pltpu.VMEM((n_col, snps // FOLD, FOLD), jnp.float32),
            pltpu.VMEM((minor, snps // FOLD, FOLD), jnp.float32),
            pltpu.VMEM((major, snps // FOLD, FOLD), jnp.float32),
            pltpu.SMEM(counts.shape, jnp.int32),
            pltpu.SMEM(affected.shape[::-1], jnp.int32),
            dma((6,)),
            dma((3,)),
            pltpu.SemaphoreType.REGULAR((max(1, major - 2),)),
            dma((chips - 1, pieces)),
            dma((chips - 1, pieces)),
            dma((1,)),
            dma((n_row, NEW_CHUNKS)),
            dma((1,)),
        ],
        compiler_params=pltpu.CompilerParams(
            collective_id=0, has_side_effects=True, vmem_limit_bytes=50 * 1024 * 1024
        ),
    )(new_dosage, old_dosage, grm, counts, affected.T)
    size = old_rows - offs[LATE]
    return pl.pallas_call(
        functools.partial(finish, n_row, n_col),
        out_shape=jax.ShapeDtypeStruct(grm.shape, grm.dtype),
        in_specs=[vmem] * 4,
        out_specs=hbm,
        scratch_shapes=[
            pltpu.VMEM(((chips - 1) * CORES * size, out_cols), jnp.bfloat16),
            dma((1,)),
        ],
        compiler_params=pltpu.CompilerParams(vmem_limit_bytes=12 * 1024 * 1024),
    )(res, old_buf, new_buf, gain)


def solution(mesh):
    return jax.shard_map(
        on_device,
        mesh=mesh,
        in_specs=(
            P(("col", "row"), None),
            P(("row", "col"), None),
            P("row", "col"),
            P("col"),
            P("row", "col"),
        ),
        out_specs=P("row", "col"),
        check_vma=False,
    )
```

```python
import functools

import jax
import jax.numpy as jnp
from jax import lax
from jax.experimental import pallas as pl
from jax.experimental.pallas import tpu as pltpu
from jax.sharding import PartitionSpec as P

MESH = pl.DeviceIdType.MESH
CORES = 2
SPLIT = (4, 4, 4, 2, 2)
CODED = 3
LATE = 3
NEW_CHUNKS = 2
FOLD = 128
LEVELS = 32767
STRIP = 32


def sizes_of(n_row, n_col, new_rows, old_rows):
    minor = 1 << ((n_row.bit_length() - 1) // 2)
    whole = sum(SPLIT)
    offs = [old_rows * sum(SPLIT[:k]) // whole for k in range(len(SPLIT) + 1)]
    return minor, n_row // minor, n_col // CORES, offs


def ds(start, size, step):
    return pl.ds(pl.multiple_of(start, step), size)


def slot_place(a, major, t):
    near = jnp.minimum(a, major - 1 - a)
    step = (t + 1) // 2
    toward = jnp.where(a > major - 1 - a, step, -step)
    both = a + toward if t % 2 else a - toward
    left = a - (t - near)
    right = a + (t - near)
    one = jnp.where(a > major - 1 - a, left, right)
    return jnp.where(t <= 2 * near, both, one) if t else a


def kernel(
    n_row, n_col, new_hbm, old_hbm, grm_hbm, counts_hbm, affected_hbm,
    res, old_buf, new_buf, gain,
    new_in, old_in, new_code, old_code, part, part_y, part_z, counts, affected,
    load_sem, sum_recv, far, x_recv, sib_recv, own_recv, new_recv, sent,
):
    snps = new_in.shape[1]
    new_rows, old_rows = new_in.shape[0], old_in.shape[0]
    out_rows, out_cols = res.shape
    tile = out_cols // counts.shape[0]
    minor, major, chips, offs = sizes_of(n_row, n_col, new_rows, old_rows)
    pieces = len(offs) - 1
    new_chunk = new_rows // NEW_CHUNKS
    final = NEW_CHUNKS - 1
    group = minor * new_rows
    folds = snps // FOLD
    unit = new_chunk

    row, col = lax.axis_index("row"), lax.axis_index("col")
    a, b = row // minor, row % minor
    chip, core = col // CORES, col % CORES
    sibling = chip * CORES + (CORES - 1 - core)
    has_left, has_right = a > 0, a < major - 1

    def span(k):
        return offs[k + 1] - offs[k]

    grain = min(span(k) for k in range(pieces))

    old_load = pltpu.make_async_copy(old_hbm, old_in, load_sem.at[0])
    new_load = pltpu.make_async_copy(new_hbm, new_in, load_sem.at[1])
    grm_load = pltpu.make_async_copy(grm_hbm, res, load_sem.at[2])
    counts_load = pltpu.make_async_copy(counts_hbm, counts, load_sem.at[3])
    affected_load = pltpu.make_async_copy(affected_hbm, affected, load_sem.at[4])
    old_load.start()
    new_load.start()
    counts_load.start()
    affected_load.start()

    barrier = pltpu.get_barrier_semaphore()

    def greet(device):
        pl.semaphore_signal(barrier, inc=1, device_id=device, device_id_type=MESH)

    for d in range(1, n_col):
        greet((row, (col + d) % n_col))
    for d in range(1, minor):
        greet((a * minor + (b + d) % minor, col))

    @pl.when(has_left)
    def _():
        greet((row - minor, col))

    @pl.when(has_right)
    def _():
        greet((row + minor, col))

    def score_place(j, k):
        return j // CORES * (CORES * old_rows) + CORES * offs[k] + j % CORES * span(k)

    def code_place(j, k):
        return j // CORES * (CORES * offs[CODED]) + CORES * offs[k] + j % CORES * span(k)

    def exact_part(j, k):
        return old_buf.at[ds(score_place(j, k), span(k), grain), :]

    def old_part(j, k):
        if k < CODED:
            return old_code.at[ds(code_place(j, k), span(k), grain), :]
        return exact_part(j, k)

    own_start = col * old_rows

    def own_part(k):
        if k < CODED:
            return old_part(col, k)
        return old_buf.at[ds(own_start + offs[k], span(k), grain), :]

    def new_part(r, k):
        return new_code.at[ds(r * new_rows + k * new_chunk, new_chunk, new_chunk), :]

    def far_copy(k, d):
        return pltpu.make_async_remote_copy(
            own_part(k), old_part(col, k), sent.at[0], x_recv.at[chips - d - 1, k],
            device_id=(row, (chip + d) % chips * CORES + core), device_id_type=MESH,
        )

    def far_taken(k, d):
        j = (chip + d) % chips * CORES + core
        return pltpu.make_async_remote_copy(
            old_part(j, k), old_part(j, k), sent.at[0], x_recv.at[d - 1, k],
            device_id=(row, j), device_id_type=MESH,
        )

    def pass_copy(k, d, which):
        j = (chip + d) % chips * CORES + which
        return pltpu.make_async_remote_copy(
            old_part(j, k), old_part(j, k), sent.at[0], sib_recv.at[d - 1, k],
            device_id=(row, sibling), device_id_type=MESH,
        )

    def own_copy(j):
        part_of = old_buf.at[ds(j * old_rows, old_rows, grain), :]
        return pltpu.make_async_remote_copy(
            part_of, part_of, sent.at[0], own_recv.at[0],
            device_id=(row, sibling), device_id_type=MESH,
        )

    def new_copy(r, k, to):
        return pltpu.make_async_remote_copy(
            new_part(r, k), new_part(r, k), sent.at[0], new_recv.at[r, k],
            device_id=(to, col), device_id_type=MESH,
        )

    sends = []

    def start(copy, cond=None):
        if cond is None:
            copy.start()
        else:
            @pl.when(cond)
            def _():
                copy.start()
        sends.append((cond, copy))

    def is_end(z):
        return (z == 0) | (z == major - 1)

    def encode(x):
        return ((x * LEVELS + 0.5).astype(jnp.int32) - LEVELS).astype(jnp.int16)

    def encode_old(k):
        old_code[ds(code_place(col, k), span(k), grain), :] = encode(
            old_in[offs[k]:offs[k + 1], :]
        )

    def send_sums(buf, me, count, recv, target):
        for d in range(1, count):
            copy = pltpu.make_async_remote_copy(
                buf.at[me], buf.at[me], sent.at[0], recv,
                device_id=target((me + d) % count), device_id_type=MESH,
            )
            start(copy)

    def take_sums(buf, me, count, recv, target):
        rest = buf.at[pl.ds(0, count - 1)]
        pltpu.make_async_copy(rest, rest, recv).wait()
        total = buf[0]
        for i in range(1, count):
            total = total + buf[i]
        return total

    over_col = (part, col, n_col, sum_recv.at[0], lambda i: (row, i))
    over_mid = (part_y, b, minor, sum_recv.at[1], lambda i: (a * minor + i, col))
    over_row = (part_z, a, major, sum_recv.at[2], lambda i: (i * minor + b, col))

    def far_tell(h):
        @pl.when(has_right & (a - (h - 1) >= 0))
        def _():
            pl.semaphore_signal(
                far.at[h - 2], inc=1, device_id=(row + minor, col), device_id_type=MESH
            )

        @pl.when(has_left & (a + (h - 1) <= major - 1))
        def _():
            pl.semaphore_signal(
                far.at[h - 2], inc=1, device_id=(row - minor, col), device_id_type=MESH
            )

    def far_hear(h):
        heard = (a - h >= 0).astype(jnp.int32) + (a + h <= major - 1).astype(jnp.int32)

        @pl.when(heard > 0)
        def _():
            pl.semaphore_wait(far.at[h - 2], heard)

    def send_z(k):
        start(new_copy(row, k, row + minor), has_right)
        start(new_copy(row, k, row - minor), has_left)

    def send_y(z, k, cond=None):
        for d in range(1, minor):
            start(new_copy(z * minor + b, k, a * minor + (b + d) % minor), cond)

    def send_old(k):
        for d in range(1, chips):
            start(far_copy(k, d))

    with jax.named_scope("loadold"):
        old_load.wait()
        mine = jnp.sum(old_in[...], axis=0, keepdims=True)
        for f in range(folds):
            part[pl.ds(col, 1), f, :] = mine[:, f * FOLD:(f + 1) * FOLD]
    with jax.named_scope("barrier"):
        pl.semaphore_wait(
            barrier,
            n_col - 1 + minor - 1 + has_left.astype(jnp.int32) + has_right.astype(jnp.int32),
        )
    send_sums(*over_col)
    encode_old(0)
    send_old(0)
    far_tell(2)
    with jax.named_scope("first"):
        new_load.wait()
        new_code[ds(row * new_rows, new_rows, new_rows), :] = encode(new_in[...])
        send_z(0)
        send_y(a, 0)
        grm_load.start()
        for k in range(1, CODED):
            encode_old(k)
            send_old(k)
        for k in range(1, NEW_CHUNKS):
            send_z(k)
    with jax.named_scope("sumcol"):
        part_y[b] = take_sums(*over_col)
        send_sums(*over_mid)
        for k in range(1, NEW_CHUNKS):
            send_y(a, k)
    with jax.named_scope("hear"):
        for h in range(2, major):
            far_hear(h)
            if h + 1 < major:
                far_tell(h + 1)
    with jax.named_scope("sumy"):
        part_z[a] = take_sums(*over_mid)
        send_sums(*over_row)


    def sided(s):
        for left in (True, False):
            z = a - 1 - s if left else a + 1 + s
            valid = z >= 0 if left else z < major
            onward = valid & (has_right if left else has_left)
            dest = row + minor if left else row - minor
            yield z, valid, onward, dest

    def relay(s, k):
        for z, valid, onward, dest in sided(s):
            r = z * minor + b

            @pl.when(valid)
            def _():
                new_copy(r, k, row).wait_recv()
            start(new_copy(r, k, dest), onward)
            across = valid & jnp.logical_not(is_end(z)) if k == final else valid
            send_y(z, k, across)

    def relay_first(s):
        for z, valid, onward, dest in sided(s):
            for d in range(1, minor):
                r = z * minor + (b + d) % minor

                @pl.when(valid & is_end(z))
                def _():
                    new_copy(r, final, row).wait_recv()
                start(new_copy(r, final, dest), onward & is_end(z))

    def own_first():
        for d in range(1, minor):
            r = a * minor + (b + d) % minor
            new_copy(r, final, row).wait_recv()
            start(new_copy(r, final, row + minor), a == 0)
            start(new_copy(r, final, row - minor), a == major - 1)

    def wait_y(t):
        z = slot_place(a, major, t)
        for k in range(NEW_CHUNKS):
            if t == 0 and k == final:
                continue
            for d in range(1, minor):
                r = z * minor + (b + d) % minor
                copy = new_copy(r, k, row)
                if k < final:
                    copy.wait_recv()
                else:
                    @pl.when(jnp.logical_not(is_end(z)))
                    def _():
                        copy.wait_recv()

    def forward_old(k):
        for d in range(1, chips):
            far_taken(k, d).wait_recv()
            start(pass_copy(k, d, core))

    def wait_sib_own():
        own_copy(sibling).wait_recv()

    def wait_sib_forwarded(k):
        for d in range(1, chips):
            pass_copy(k, d, CORES - 1 - core).wait_recv()

    def add(rows, z, product, row_tile):
        cols = ds(z * group, group, group)
        mark = affected[(z * group) // tile, row_tile].astype(jnp.float32)
        res[rows, cols] = (
            res[rows, cols].astype(jnp.float32) + product * (mark / snps)
        ).astype(jnp.bfloat16)

    def product_of(first, height, step, t0, tn):
        return lax.dot_general(
            old_buf[ds(first, height, step), :], new_buf[t0 * group:(t0 + tn) * group, :],
            (((1,), (1,)), ((), ())), preferred_element_type=jnp.float32,
        )

    def block(where, k0, k1, t0, tn):
        low = CORES * offs[k0]
        height = CORES * (offs[k1] - offs[k0])
        product = product_of(where * CORES * old_rows + low, height, grain, t0, tn)
        for i in range(tn):
            z = slot_place(a, major, t0 + i)
            for k in range(k0, k1):
                for c in range(CORES):
                    first = (where * CORES + c) * old_rows + offs[k]
                    at = CORES * offs[k] - low + c * span(k)
                    add(
                        ds(first, span(k), grain), z,
                        product[at:at + span(k), i * group:(i + 1) * group], first // tile,
                    )

    def local_rows(t0, tn):
        step = min(tile, CORES * old_rows)

        @pl.loop(0, CORES * old_rows // step)
        def _(i):
            first = chip * CORES * old_rows + i * step
            product = product_of(first, step, step, t0, tn)
            for j in range(tn):
                add(
                    ds(first, step, step), slot_place(a, major, t0 + j),
                    product[:, j * group:(j + 1) * group], first // tile,
                )

    def far_rows(k0, k1, t0, tn):
        for d in range(1, chips):
            block((chip + d) % chips, k0, k1, t0, tn)

    with jax.named_scope("relay0"):
        relay(0, 0)
    with jax.named_scope("relay1"):
        for k in range(1, NEW_CHUNKS):
            relay(0, k)
    with jax.named_scope("own_first"):
        own_first()
    with jax.named_scope("x0"):
        forward_old(0)
    with jax.named_scope("sumz"):
        total = take_sums(*over_row)
    totals = jnp.concatenate([total[f:f + 1] for f in range(folds)], axis=1)
    doubled = totals / (old_rows * n_row * n_col)
    inverse = 1.0 / jnp.sqrt(doubled * (1.0 - 0.5 * doubled) + 0.1)
    code_scale = inverse / LEVELS
    code_shift = (1.0 - doubled) * inverse

    def score(k):
        old_buf[ds(own_start + offs[k], span(k), grain), :] = (
            (old_in[offs[k]:offs[k + 1], :] - doubled) * inverse
        ).astype(jnp.bfloat16)

    with jax.named_scope("score"):
        for k in range(CODED, pieces):
            score(k)
            send_old(k)
        for k in range(CODED):
            score(k)
        start(own_copy(col))
        counts_load.wait()
        affected_load.wait()
        grm_load.wait()

    def decode(codes):
        return codes.astype(jnp.int32).astype(jnp.float32) * code_scale + code_shift

    def decode_new(t):
        z = slot_place(a, major, t)
        count = counts[(z * group) // tile]

        @pl.loop(0, group // STRIP)
        def _(i):
            at = z * group + i * STRIP
            place = lax.broadcasted_iota(jnp.int32, (STRIP, 1), 0) + at % tile
            usable = (place < count).astype(jnp.float32)
            codes = new_code[ds(at, STRIP, STRIP), :]
            new_buf[ds(t * group + i * STRIP, STRIP, STRIP), :] = (
                decode(codes) * usable
            ).astype(jnp.bfloat16)

    def decode_old(k):
        if k >= CODED:
            return
        strip = min(STRIP, CORES * span(k))
        for d in range(1, chips):
            j = (chip + d) % chips * CORES

            @pl.loop(0, CORES * span(k) // strip)
            def _(i):
                codes = old_code[ds(code_place(j, k) + i * strip, strip, strip), :]
                old_buf[ds(score_place(j, k) + i * strip, strip, strip), :] = (
                    decode(codes).astype(jnp.bfloat16)
                )

    def take_group(t):
        with jax.named_scope("wy%d" % t):
            wait_y(t)
        with jax.named_scope("dec%d" % t):
            decode_new(t)

    def take_old(k):
        with jax.named_scope("ws%d" % k):
            wait_sib_forwarded(k)
            decode_old(k)

    with jax.named_scope("gain"):
        for i in range(out_rows // tile):
            for j in range(out_cols // tile):
                mark = affected[j, i].astype(jnp.float32)
                gain[i:i + 1, j * tile:(j + 1) * tile] = jnp.full(
                    (1, tile), mark / snps, jnp.float32
                )

    def relayed(s, k):
        with jax.named_scope("relay%d_%d" % (s, k)):
            relay(s, k)

    def relayed_first(s):
        with jax.named_scope("first%d" % s):
            relay_first(s)

    def forwarded(k):
        with jax.named_scope("x%d" % k):
            forward_old(k)

    def local(t0, tn):
        with jax.named_scope("mm_local%d" % t0):
            local_rows(t0, tn)

    def distant(k0, k1, t0, tn):
        with jax.named_scope("mm_far%d_%d" % (k0, t0)):
            far_rows(k0, k1, t0, tn)

    take_group(0)
    take_old(0)
    relayed(1, 0)
    relayed_first(0)
    with jax.named_scope("sibown"):
        wait_sib_own()
    local(0, 1)
    relayed(1, 1)
    forwarded(1)
    distant(0, 1, 0, 1)
    take_group(1)
    local(1, 1)
    distant(0, 1, 1, 1)
    for s in range(2, major - 1):
        relayed(s, 0)
        relayed_first(s - 1)
        if s == 2:
            take_old(1)
            distant(1, 2, 0, 2)
            forwarded(2)
        relayed(s, 1)
    for t in range(2, major - 1):
        take_group(t)
        local(t, 1)
        distant(0, 2, t, 1)
    take_old(2)
    distant(2, LATE, 0, major - 1)
    forwarded(3)
    relayed_first(major - 2)
    take_group(major - 1)
    local(major - 1, 1)
    for k in range(4, pieces):
        forwarded(k)
    distant(0, LATE, major - 1, 1)
    for k in range(LATE, pieces):
        take_old(k)

    with jax.named_scope("sends"):
        for cond, copy in sends:
            if cond is None:
                copy.wait_send()
            else:
                @pl.when(cond)
                def _():
                    copy.wait_send()


def finish(n_row, n_col, res, old_buf, new_buf, gain, out_hbm, stage, sem):
    out_rows, out_cols = res.shape
    old_rows, new_rows = out_rows // n_col, out_cols // n_row
    minor, major, chips, offs = sizes_of(n_row, n_col, new_rows, old_rows)
    group = minor * new_rows
    tile = out_rows // gain.shape[0]
    early, size = offs[LATE], old_rows - offs[LATE]
    grain = min(hi - lo for lo, hi in zip(offs[:-1], offs[1:], strict=True))
    row, col = lax.axis_index("row"), lax.axis_index("col")
    a, chip = row // minor, col // CORES

    def out_copy(src, start, count):
        return pltpu.make_async_copy(
            src, out_hbm.at[ds(start, count, grain), :], sem.at[0]
        )

    mine = chip * CORES * old_rows
    copies = [
        out_copy(res.at[ds(mine, CORES * old_rows, grain), :], mine, CORES * old_rows)
    ]
    for d in range(1, chips):
        for c in range(CORES):
            first = ((chip + d) % chips * CORES + c) * old_rows
            copies.append(out_copy(res.at[ds(first, early, grain), :], first, early))
    for copy in copies:
        copy.start()
    with jax.named_scope("tail"):
        for d in range(1, chips):
            where = (chip + d) % chips
            low = where * CORES * old_rows + CORES * early
            product = lax.dot_general(
                old_buf[ds(low, CORES * size, grain), :], new_buf[...],
                (((1,), (1,)), ((), ())), preferred_element_type=jnp.float32,
            )
            for c in range(CORES):
                start_row = (where * CORES + c) * old_rows + early
                to = ((d - 1) * CORES + c) * size
                for k in range(LATE, len(offs) - 1):
                    span = offs[k + 1] - offs[k]
                    at = CORES * (offs[k] - early) + c * span
                    lead = offs[k] - early
                    first = start_row + lead
                    for t in range(major):
                        cols = ds(slot_place(a, major, t) * group, group, group)
                        stage[to + lead:to + lead + span, cols] = (
                            res[ds(first, span, grain), cols].astype(jnp.float32)
                            + product[at:at + span, t * group:(t + 1) * group]
                            * gain[pl.ds(first // tile, 1), cols]
                        ).astype(jnp.bfloat16)
                copy = out_copy(stage.at[pl.ds(to, size), :], start_row, size)
                copy.start()
                copies.append(copy)
    with jax.named_scope("out"):
        for copy in copies:
            copy.wait()


def on_device(new_dosage, old_dosage, grm, counts, affected):
    n_row, n_col = lax.axis_size("row"), lax.axis_size("col")
    new_rows, snps = new_dosage.shape
    old_rows = old_dosage.shape[0]
    out_rows, out_cols = grm.shape
    minor, major, chips, offs = sizes_of(n_row, n_col, new_rows, old_rows)
    pieces = len(offs) - 1
    dma = pltpu.SemaphoreType.DMA
    hbm = pl.BlockSpec(memory_space=pltpu.HBM)
    vmem = pl.BlockSpec(memory_space=pltpu.VMEM)
    row_tiles = affected.shape[0]
    res, old_buf, new_buf, gain = pl.pallas_call(
        functools.partial(kernel, n_row, n_col),
        out_shape=(
            pltpu.VMEM(grm.shape, grm.dtype),
            pltpu.VMEM((old_rows * n_col, snps), jnp.bfloat16),
            pltpu.VMEM((new_rows * n_row, snps), jnp.bfloat16),
            pltpu.VMEM((row_tiles, out_cols), jnp.float32),
        ),
        in_specs=[hbm] * 5,
        out_specs=(vmem,) * 4,
        scratch_shapes=[
            pltpu.VMEM((new_rows, snps), jnp.float32),
            pltpu.VMEM((old_rows, snps), jnp.float32),
            pltpu.VMEM((new_rows * n_row, snps), jnp.int16),
            pltpu.VMEM((offs[CODED] * n_col, snps), jnp.int16),
            pltpu.VMEM((n_col, snps // FOLD, FOLD), jnp.float32),
            pltpu.VMEM((minor, snps // FOLD, FOLD), jnp.float32),
            pltpu.VMEM((major, snps // FOLD, FOLD), jnp.float32),
            pltpu.SMEM(counts.shape, jnp.int32),
            pltpu.SMEM(affected.shape[::-1], jnp.int32),
            dma((5,)),
            dma((3,)),
            pltpu.SemaphoreType.REGULAR((max(1, major - 2),)),
            dma((chips - 1, pieces)),
            dma((chips - 1, pieces)),
            dma((1,)),
            dma((n_row, NEW_CHUNKS)),
            dma((1,)),
        ],
        compiler_params=pltpu.CompilerParams(
            collective_id=0, has_side_effects=True, vmem_limit_bytes=50 * 1024 * 1024
        ),
    )(new_dosage, old_dosage, grm, counts, affected.T)
    size = old_rows - offs[LATE]
    return pl.pallas_call(
        functools.partial(finish, n_row, n_col),
        out_shape=jax.ShapeDtypeStruct(grm.shape, grm.dtype),
        in_specs=[vmem] * 4,
        out_specs=hbm,
        scratch_shapes=[
            pltpu.VMEM(((chips - 1) * CORES * size, out_cols), jnp.bfloat16),
            dma((1,)),
        ],
        compiler_params=pltpu.CompilerParams(vmem_limit_bytes=12 * 1024 * 1024),
    )(res, old_buf, new_buf, gain)


def solution(mesh):
    return jax.shard_map(
        on_device,
        mesh=mesh,
        in_specs=(
            P(("col", "row"), None),
            P(("row", "col"), None),
            P("row", "col"),
            P("col"),
            P("row", "col"),
        ),
        out_specs=P("row", "col"),
        check_vma=False,
    )
```

```python
import functools

import jax
import jax.numpy as jnp
from jax import lax
from jax.experimental import pallas as pl
from jax.experimental.pallas import tpu as pltpu
from jax.sharding import PartitionSpec as P

MESH = pl.DeviceIdType.MESH
CORES = 2
SPLIT = (4, 2, 4, 4, 2)
AHEAD = 2
CODED = 3
LATE = 3
NEW_CHUNKS = 2
FOLD = 128
LEVELS = 32767
STRIP = 32


def sizes_of(n_row, n_col, new_rows, old_rows):
    minor = 1 << ((n_row.bit_length() - 1) // 2)
    whole = sum(SPLIT)
    offs = [old_rows * sum(SPLIT[:k]) // whole for k in range(len(SPLIT) + 1)]
    return minor, n_row // minor, n_col // CORES, offs


def ds(start, size, step):
    return pl.ds(pl.multiple_of(start, step), size)


def slot_place(a, major, t):
    near = jnp.minimum(a, major - 1 - a)
    step = (t + 1) // 2
    toward = jnp.where(a > major - 1 - a, step, -step)
    both = a + toward if t % 2 else a - toward
    left = a - (t - near)
    right = a + (t - near)
    one = jnp.where(a > major - 1 - a, left, right)
    return jnp.where(t <= 2 * near, both, one) if t else a


def kernel(
    n_row, n_col, new_hbm, old_hbm, grm_hbm, counts_hbm, affected_hbm,
    res, old_buf, new_buf, gain,
    new_in, old_in, new_code, old_code, part, part_y, part_z, counts, affected,
    load_sem, sum_recv, far, x_recv, sib_recv, own_recv, new_recv, sent,
):
    snps = new_in.shape[1]
    new_rows, old_rows = new_in.shape[0], old_in.shape[0]
    out_rows, out_cols = res.shape
    tile = out_cols // counts.shape[0]
    minor, major, chips, offs = sizes_of(n_row, n_col, new_rows, old_rows)
    pieces = len(offs) - 1
    last = pieces - 1
    new_chunk = new_rows // NEW_CHUNKS
    final = NEW_CHUNKS - 1
    group = minor * new_rows
    folds = snps // FOLD
    unit = new_chunk

    row, col = lax.axis_index("row"), lax.axis_index("col")
    a, b = row // minor, row % minor
    chip, core = col // CORES, col % CORES
    sibling = chip * CORES + (CORES - 1 - core)
    has_left, has_right = a > 0, a < major - 1

    def span(k):
        return offs[k + 1] - offs[k]

    grain = min(span(k) for k in range(pieces))

    old_loads = [
        pltpu.make_async_copy(
            old_hbm.at[pl.ds(lo, hi - lo), :], old_in.at[pl.ds(lo, hi - lo), :], load_sem.at[i]
        )
        for i, (lo, hi) in enumerate(((0, offs[1]), (offs[1], old_rows)))
    ]
    new_load = pltpu.make_async_copy(new_hbm, new_in, load_sem.at[2])
    grm_load = pltpu.make_async_copy(grm_hbm, res, load_sem.at[3])
    counts_load = pltpu.make_async_copy(counts_hbm, counts, load_sem.at[4])
    affected_load = pltpu.make_async_copy(affected_hbm, affected, load_sem.at[5])
    old_loads[0].start()
    new_load.start()
    old_loads[1].start()
    counts_load.start()
    affected_load.start()

    barrier = pltpu.get_barrier_semaphore()

    def greet(device):
        pl.semaphore_signal(barrier, inc=1, device_id=device, device_id_type=MESH)

    for d in range(1, n_col):
        greet((row, (col + d) % n_col))
    for d in range(1, minor):
        greet((a * minor + (b + d) % minor, col))

    @pl.when(has_left)
    def _():
        greet((row - minor, col))

    @pl.when(has_right)
    def _():
        greet((row + minor, col))

    def score_place(j, k):
        return j // CORES * (CORES * old_rows) + CORES * offs[k] + j % CORES * span(k)

    def code_place(j, k):
        return j // CORES * (CORES * offs[CODED]) + CORES * offs[k] + j % CORES * span(k)

    def exact_part(j, k):
        return old_buf.at[ds(score_place(j, k), span(k), grain), :]

    def old_part(j, k):
        if k < CODED:
            return old_code.at[ds(code_place(j, k), span(k), grain), :]
        return exact_part(j, k)

    own_start = col * old_rows

    def own_part(k):
        if k < CODED:
            return old_part(col, k)
        return old_buf.at[ds(own_start + offs[k], span(k), grain), :]

    def new_part(r, k):
        return new_code.at[ds(r * new_rows + k * new_chunk, new_chunk, new_chunk), :]

    def far_copy(k, d):
        return pltpu.make_async_remote_copy(
            own_part(k), old_part(col, k), sent.at[0], x_recv.at[chips - d - 1, k],
            device_id=(row, (chip + d) % chips * CORES + core), device_id_type=MESH,
        )

    def far_taken(k, d):
        j = (chip + d) % chips * CORES + core
        return pltpu.make_async_remote_copy(
            old_part(j, k), old_part(j, k), sent.at[0], x_recv.at[d - 1, k],
            device_id=(row, j), device_id_type=MESH,
        )

    def pass_copy(k, d, which):
        j = (chip + d) % chips * CORES + which
        return pltpu.make_async_remote_copy(
            old_part(j, k), old_part(j, k), sent.at[0], sib_recv.at[d - 1, k],
            device_id=(row, sibling), device_id_type=MESH,
        )

    def own_copy(j):
        part_of = old_buf.at[ds(j * old_rows, old_rows, grain), :]
        return pltpu.make_async_remote_copy(
            part_of, part_of, sent.at[0], own_recv.at[0],
            device_id=(row, sibling), device_id_type=MESH,
        )

    def new_copy(r, k, to):
        return pltpu.make_async_remote_copy(
            new_part(r, k), new_part(r, k), sent.at[0], new_recv.at[r, k],
            device_id=(to, col), device_id_type=MESH,
        )

    sends = []

    def start(copy, cond=None):
        if cond is None:
            copy.start()
        else:
            @pl.when(cond)
            def _():
                copy.start()
        sends.append((cond, copy))

    def is_end(z):
        return (z == 0) | (z == major - 1)

    def encode(x):
        return ((x * LEVELS + 0.5).astype(jnp.int32) - LEVELS).astype(jnp.int16)

    def encode_old(k):
        old_code[ds(code_place(col, k), span(k), grain), :] = encode(
            old_in[offs[k]:offs[k + 1], :]
        )

    def send_sums(buf, me, count, recv, target):
        for d in range(1, count):
            copy = pltpu.make_async_remote_copy(
                buf.at[me], buf.at[me], sent.at[0], recv,
                device_id=target((me + d) % count), device_id_type=MESH,
            )
            start(copy)

    def take_sums(buf, me, count, recv, target):
        rest = buf.at[pl.ds(0, count - 1)]
        pltpu.make_async_copy(rest, rest, recv).wait()
        total = buf[0]
        for i in range(1, count):
            total = total + buf[i]
        return total

    over_col = (part, col, n_col, sum_recv.at[0], lambda i: (row, i))
    over_mid = (part_y, b, minor, sum_recv.at[1], lambda i: (a * minor + i, col))
    over_row = (part_z, a, major, sum_recv.at[2], lambda i: (i * minor + b, col))

    def far_tell(h):
        @pl.when(has_right & (a - (h - 1) >= 0))
        def _():
            pl.semaphore_signal(
                far.at[h - 2], inc=1, device_id=(row + minor, col), device_id_type=MESH
            )

        @pl.when(has_left & (a + (h - 1) <= major - 1))
        def _():
            pl.semaphore_signal(
                far.at[h - 2], inc=1, device_id=(row - minor, col), device_id_type=MESH
            )

    def far_hear(h):
        heard = (a - h >= 0).astype(jnp.int32) + (a + h <= major - 1).astype(jnp.int32)

        @pl.when(heard > 0)
        def _():
            pl.semaphore_wait(far.at[h - 2], heard)

    def send_z(k):
        start(new_copy(row, k, row + minor), has_right)
        start(new_copy(row, k, row - minor), has_left)

    def send_y(z, k, cond=None):
        for d in range(1, minor):
            start(new_copy(z * minor + b, k, a * minor + (b + d) % minor), cond)

    lender = core == CORES - 1
    taker = core != CORES - 1

    def send_old(k):
        for d in range(1, chips):
            start(far_copy(k, d), lender if k == last else None)

    def lend(d, which):
        j = (chip + d) % chips * CORES + which
        return pltpu.make_async_remote_copy(
            exact_part(j, last), exact_part(j, last), sent.at[0], x_recv.at[d - 1, pieces],
            device_id=(row, j), device_id_type=MESH,
        )

    def send_lent():
        for d in range(1, chips):
            copy = pltpu.make_async_remote_copy(
                old_buf.at[ds(sibling * old_rows + offs[last], span(last), grain), :],
                exact_part(sibling, last), sent.at[0], x_recv.at[chips - d - 1, pieces],
                device_id=(row, (chip + d) % chips * CORES + core), device_id_type=MESH,
            )
            start(copy, lender)

    def pass_lent(d, which):
        j = (chip + d) % chips * CORES + which
        return pltpu.make_async_remote_copy(
            exact_part(j, last), exact_part(j, last), sent.at[0], sib_recv.at[d - 1, pieces],
            device_id=(row, sibling), device_id_type=MESH,
        )

    with jax.named_scope("load0"):
        old_loads[0].wait()
        encode_old(0)
        new_load.wait()
        new_code[ds(row * new_rows, new_rows, new_rows), :] = encode(new_in[...])
    with jax.named_scope("barrier"):
        pl.semaphore_wait(
            barrier,
            n_col - 1 + minor - 1 + has_left.astype(jnp.int32) + has_right.astype(jnp.int32),
        )
    send_old(0)
    send_z(0)
    far_tell(2)
    with jax.named_scope("loadold"):
        old_loads[1].wait()
        mine = jnp.sum(old_in[...], axis=0, keepdims=True)
        for f in range(folds):
            part_y[pl.ds(b, 1), f, :] = mine[:, f * FOLD:(f + 1) * FOLD]
        send_sums(*over_mid)
    with jax.named_scope("first"):
        for k in range(NEW_CHUNKS):
            send_y(a, k)
        for k in range(1, CODED):
            encode_old(k)
        for k in range(1, AHEAD):
            send_old(k)
        grm_load.start()
    with jax.named_scope("hear"):
        for h in range(2, major):
            far_hear(h)
            if h + 1 < major:
                far_tell(h + 1)
    with jax.named_scope("sumy"):
        part_z[a] = take_sums(*over_mid)
        send_sums(*over_row)
        for k in range(1, NEW_CHUNKS):
            send_z(k)

    def sided(s):
        for left in (True, False):
            z = a - 1 - s if left else a + 1 + s
            valid = z >= 0 if left else z < major
            onward = valid & (has_right if left else has_left)
            dest = row + minor if left else row - minor
            yield z, valid, onward, dest

    def relay(s, k):
        for z, valid, onward, dest in sided(s):
            r = z * minor + b

            @pl.when(valid)
            def _():
                new_copy(r, k, row).wait_recv()
            start(new_copy(r, k, dest), onward)
            across = valid & jnp.logical_not(is_end(z)) if k == final else valid
            send_y(z, k, across)

    def relay_first(s):
        for z, valid, onward, dest in sided(s):
            for d in range(1, minor):
                r = z * minor + (b + d) % minor

                @pl.when(valid & is_end(z))
                def _():
                    new_copy(r, final, row).wait_recv()
                start(new_copy(r, final, dest), onward & is_end(z))

    def own_first():
        for d in range(1, minor):
            r = a * minor + (b + d) % minor
            new_copy(r, final, row).wait_recv()
            start(new_copy(r, final, row + minor), a == 0)
            start(new_copy(r, final, row - minor), a == major - 1)

    def wait_y(t):
        z = slot_place(a, major, t)
        for k in range(NEW_CHUNKS):
            if t == 0 and k == final:
                continue
            for d in range(1, minor):
                r = z * minor + (b + d) % minor
                copy = new_copy(r, k, row)
                if k < final:
                    copy.wait_recv()
                else:
                    @pl.when(jnp.logical_not(is_end(z)))
                    def _():
                        copy.wait_recv()

    def forward_old(k):
        for d in range(1, chips):
            if k < last:
                far_taken(k, d).wait_recv()
                start(pass_copy(k, d, core))
            else:
                @pl.when(lender)
                def _():
                    far_taken(k, d).wait_recv()
                start(pass_copy(k, d, core), lender)

                @pl.when(lender)
                def _():
                    lend(d, CORES - 1 - core).wait_recv()
                start(pass_lent(d, CORES - 1 - core), lender)

    def wait_sib_own():
        own_copy(sibling).wait_recv()

    def wait_sib_forwarded(k):
        for d in range(1, chips):
            if k < last:
                pass_copy(k, d, CORES - 1 - core).wait_recv()
            else:
                @pl.when(taker)
                def _():
                    pass_copy(k, d, CORES - 1 - core).wait_recv()
                    pass_lent(d, core).wait_recv()

    def add(rows, z, product, row_tile):
        cols = ds(z * group, group, group)
        mark = affected[(z * group) // tile, row_tile].astype(jnp.float32)
        res[rows, cols] = (
            res[rows, cols].astype(jnp.float32) + product * (mark / snps)
        ).astype(jnp.bfloat16)

    def product_of(first, height, step, t0, tn):
        return lax.dot_general(
            old_buf[ds(first, height, step), :], new_buf[t0 * group:(t0 + tn) * group, :],
            (((1,), (1,)), ((), ())), preferred_element_type=jnp.float32,
        )

    def block(where, k0, k1, t0, tn):
        low = CORES * offs[k0]
        height = CORES * (offs[k1] - offs[k0])
        product = product_of(where * CORES * old_rows + low, height, grain, t0, tn)
        for i in range(tn):
            z = slot_place(a, major, t0 + i)
            for k in range(k0, k1):
                for c in range(CORES):
                    first = (where * CORES + c) * old_rows + offs[k]
                    at = CORES * offs[k] - low + c * span(k)
                    add(
                        ds(first, span(k), grain), z,
                        product[at:at + span(k), i * group:(i + 1) * group], first // tile,
                    )

    def local_rows(t0, tn):
        step = min(tile, CORES * old_rows)

        @pl.loop(0, CORES * old_rows // step)
        def _(i):
            first = chip * CORES * old_rows + i * step
            product = product_of(first, step, step, t0, tn)
            for j in range(tn):
                add(
                    ds(first, step, step), slot_place(a, major, t0 + j),
                    product[:, j * group:(j + 1) * group], first // tile,
                )

    def far_rows(k0, k1, t0, tn):
        for d in range(1, chips):
            block((chip + d) % chips, k0, k1, t0, tn)

    with jax.named_scope("relay0"):
        relay(0, 0)
    with jax.named_scope("sumz"):
        part[col] = take_sums(*over_row)
        send_sums(*over_col)
        for k in range(AHEAD, CODED):
            send_old(k)
    with jax.named_scope("relay1"):
        for k in range(1, NEW_CHUNKS):
            relay(0, k)
    with jax.named_scope("own_first"):
        own_first()
    with jax.named_scope("x0"):
        forward_old(0)
    with jax.named_scope("sumcol"):
        total = take_sums(*over_col)
    totals = jnp.concatenate([total[f:f + 1] for f in range(folds)], axis=1)
    doubled = totals / (old_rows * n_row * n_col)
    inverse = 1.0 / jnp.sqrt(doubled * (1.0 - 0.5 * doubled) + 0.1)
    code_scale = inverse / LEVELS
    code_shift = (1.0 - doubled) * inverse

    def score(k):
        old_buf[ds(own_start + offs[k], span(k), grain), :] = (
            (old_in[offs[k]:offs[k + 1], :] - doubled) * inverse
        ).astype(jnp.bfloat16)

    with jax.named_scope("score"):
        for k in range(CODED, pieces):
            score(k)
            send_old(k)
        for k in range(CODED):
            score(k)
        start(own_copy(col))
        counts_load.wait()
        affected_load.wait()
        grm_load.wait()

    def decode(codes):
        return codes.astype(jnp.int32).astype(jnp.float32) * code_scale + code_shift

    def decode_new(t):
        z = slot_place(a, major, t)
        count = counts[(z * group) // tile]

        @pl.loop(0, group // STRIP)
        def _(i):
            at = z * group + i * STRIP
            place = lax.broadcasted_iota(jnp.int32, (STRIP, 1), 0) + at % tile
            usable = (place < count).astype(jnp.float32)
            codes = new_code[ds(at, STRIP, STRIP), :]
            new_buf[ds(t * group + i * STRIP, STRIP, STRIP), :] = (
                decode(codes) * usable
            ).astype(jnp.bfloat16)

    def decode_old(k):
        if k >= CODED:
            return
        strip = min(STRIP, CORES * span(k))
        for d in range(1, chips):
            j = (chip + d) % chips * CORES

            @pl.loop(0, CORES * span(k) // strip)
            def _(i):
                codes = old_code[ds(code_place(j, k) + i * strip, strip, strip), :]
                old_buf[ds(score_place(j, k) + i * strip, strip, strip), :] = (
                    decode(codes).astype(jnp.bfloat16)
                )

    def take_group(t):
        with jax.named_scope("wy%d" % t):
            wait_y(t)
        with jax.named_scope("dec%d" % t):
            decode_new(t)

    def take_old(k):
        with jax.named_scope("ws%d" % k):
            wait_sib_forwarded(k)
            decode_old(k)

    with jax.named_scope("gain"):
        for i in range(out_rows // tile):
            for j in range(out_cols // tile):
                mark = affected[j, i].astype(jnp.float32)
                gain[i:i + 1, j * tile:(j + 1) * tile] = jnp.full(
                    (1, tile), mark / snps, jnp.float32
                )

    def relayed(s, k):
        with jax.named_scope("relay%d_%d" % (s, k)):
            relay(s, k)

    def relayed_first(s):
        with jax.named_scope("first%d" % s):
            relay_first(s)

    def forwarded(k):
        with jax.named_scope("x%d" % k):
            forward_old(k)

    def local(t0, tn):
        with jax.named_scope("mm_local%d" % t0):
            local_rows(t0, tn)

    def distant(k0, k1, t0, tn):
        with jax.named_scope("mm_far%d_%d" % (k0, t0)):
            far_rows(k0, k1, t0, tn)

    forwarded(1)
    take_group(0)
    take_old(0)
    relayed(1, 0)
    relayed_first(0)
    with jax.named_scope("sibown"):
        wait_sib_own()
        send_lent()
    local(0, 1)
    take_old(1)
    relayed(1, 1)
    distant(0, 2, 0, 1)
    take_group(1)
    local(1, 1)
    distant(0, 2, 1, 1)
    for s in range(2, major - 1):
        relayed(s, 0)
        relayed_first(s - 1)
        if s == 2:
            forwarded(2)
            take_old(2)
            distant(2, 3, 0, 2)
        relayed(s, 1)
    for t in range(2, major - 1):
        take_group(t)
        local(t, 1)
        distant(0, LATE, t, 1)
    forwarded(3)
    relayed_first(major - 2)
    take_group(major - 1)
    local(major - 1, 1)
    forwarded(4)
    distant(0, LATE, major - 1, 1)
    for k in range(LATE, pieces):
        take_old(k)

    with jax.named_scope("sends"):
        for cond, copy in sends:
            if cond is None:
                copy.wait_send()
            else:
                @pl.when(cond)
                def _():
                    copy.wait_send()


def finish(n_row, n_col, res, old_buf, new_buf, gain, out_hbm, stage, sem):
    out_rows, out_cols = res.shape
    old_rows, new_rows = out_rows // n_col, out_cols // n_row
    minor, major, chips, offs = sizes_of(n_row, n_col, new_rows, old_rows)
    group = minor * new_rows
    tile = out_rows // gain.shape[0]
    early, size = offs[LATE], old_rows - offs[LATE]
    grain = min(hi - lo for lo, hi in zip(offs[:-1], offs[1:], strict=True))
    row, col = lax.axis_index("row"), lax.axis_index("col")
    a, chip = row // minor, col // CORES

    def out_copy(src, start, count):
        return pltpu.make_async_copy(
            src, out_hbm.at[ds(start, count, grain), :], sem.at[0]
        )

    mine = chip * CORES * old_rows
    copies = [
        out_copy(res.at[ds(mine, CORES * old_rows, grain), :], mine, CORES * old_rows)
    ]
    for d in range(1, chips):
        for c in range(CORES):
            first = ((chip + d) % chips * CORES + c) * old_rows
            copies.append(out_copy(res.at[ds(first, early, grain), :], first, early))
    for copy in copies:
        copy.start()
    tails = []
    for d in range(1, chips):
        for c in range(CORES):
            to = ((d - 1) * CORES + c) * size
            start_row = ((chip + d) % chips * CORES + c) * old_rows + early
            tails.append(out_copy(stage.at[pl.ds(to, size), :], start_row, size))

    @pl.when(row >= 0)
    def _():
        for d in range(1, chips):
            where = (chip + d) % chips
            low = where * CORES * old_rows + CORES * early
            product = lax.dot_general(
                old_buf[ds(low, CORES * size, grain), :], new_buf[...],
                (((1,), (1,)), ((), ())), preferred_element_type=jnp.float32,
            )
            for c in range(CORES):
                to = ((d - 1) * CORES + c) * size
                for k in range(LATE, len(offs) - 1):
                    span = offs[k + 1] - offs[k]
                    lead = offs[k] - early
                    at = CORES * lead + c * span
                    first = (where * CORES + c) * old_rows + offs[k]
                    for t in range(major):
                        cols = ds(slot_place(a, major, t) * group, group, group)
                        stage[to + lead:to + lead + span, cols] = (
                            res[ds(first, span, grain), cols].astype(jnp.float32)
                            + product[at:at + span, t * group:(t + 1) * group]
                            * gain[pl.ds(first // tile, 1), cols]
                        ).astype(jnp.bfloat16)
                tails[(d - 1) * CORES + c].start()

    with jax.named_scope("out"):
        for copy in copies + tails:
            copy.wait()


def on_device(new_dosage, old_dosage, grm, counts, affected):
    n_row, n_col = lax.axis_size("row"), lax.axis_size("col")
    new_rows, snps = new_dosage.shape
    old_rows = old_dosage.shape[0]
    out_rows, out_cols = grm.shape
    minor, major, chips, offs = sizes_of(n_row, n_col, new_rows, old_rows)
    pieces = len(offs) - 1
    dma = pltpu.SemaphoreType.DMA
    hbm = pl.BlockSpec(memory_space=pltpu.HBM)
    vmem = pl.BlockSpec(memory_space=pltpu.VMEM)
    row_tiles = affected.shape[0]
    res, old_buf, new_buf, gain = pl.pallas_call(
        functools.partial(kernel, n_row, n_col),
        out_shape=(
            pltpu.VMEM(grm.shape, grm.dtype),
            pltpu.VMEM((old_rows * n_col, snps), jnp.bfloat16),
            pltpu.VMEM((new_rows * n_row, snps), jnp.bfloat16),
            pltpu.VMEM((row_tiles, out_cols), jnp.float32),
        ),
        in_specs=[hbm] * 5,
        out_specs=(vmem,) * 4,
        scratch_shapes=[
            pltpu.VMEM((new_rows, snps), jnp.float32),
            pltpu.VMEM((old_rows, snps), jnp.float32),
            pltpu.VMEM((new_rows * n_row, snps), jnp.int16),
            pltpu.VMEM((offs[CODED] * n_col, snps), jnp.int16),
            pltpu.VMEM((n_col, snps // FOLD, FOLD), jnp.float32),
            pltpu.VMEM((minor, snps // FOLD, FOLD), jnp.float32),
            pltpu.VMEM((major, snps // FOLD, FOLD), jnp.float32),
            pltpu.SMEM(counts.shape, jnp.int32),
            pltpu.SMEM(affected.shape[::-1], jnp.int32),
            dma((6,)),
            dma((3,)),
            pltpu.SemaphoreType.REGULAR((max(1, major - 2),)),
            dma((chips - 1, pieces + 1)),
            dma((chips - 1, pieces + 1)),
            dma((1,)),
            dma((n_row, NEW_CHUNKS)),
            dma((1,)),
        ],
        compiler_params=pltpu.CompilerParams(
            collective_id=0, has_side_effects=True, vmem_limit_bytes=50 * 1024 * 1024
        ),
    )(new_dosage, old_dosage, grm, counts, affected.T)
    size = old_rows - offs[LATE]
    return pl.pallas_call(
        functools.partial(finish, n_row, n_col),
        out_shape=jax.ShapeDtypeStruct(grm.shape, grm.dtype),
        in_specs=[vmem] * 4,
        out_specs=hbm,
        scratch_shapes=[
            pltpu.VMEM(((chips - 1) * CORES * size, out_cols), jnp.bfloat16),
            dma((1,)),
        ],
        compiler_params=pltpu.CompilerParams(vmem_limit_bytes=12 * 1024 * 1024),
    )(res, old_buf, new_buf, gain)


def solution(mesh):
    return jax.shard_map(
        on_device,
        mesh=mesh,
        in_specs=(
            P(("col", "row"), None),
            P(("row", "col"), None),
            P("row", "col"),
            P("col"),
            P("row", "col"),
        ),
        out_specs=P("row", "col"),
        check_vma=False,
    )
```

```python
import functools

import jax
import jax.numpy as jnp
from jax import lax
from jax.experimental import pallas as pl
from jax.experimental.pallas import tpu as pltpu
from jax.sharding import PartitionSpec as P

MESH = pl.DeviceIdType.MESH
CORES = 2
SPLIT = (4, 2, 4, 4, 2)
AHEAD = 2
CODED = 3
LATE = 3
NEW_CHUNKS = 2
FOLD = 128
LEVELS = 32767
STRIP = 32


def sizes_of(n_row, n_col, new_rows, old_rows):
    minor = 1 << ((n_row.bit_length() - 1) // 2)
    whole = sum(SPLIT)
    offs = [old_rows * sum(SPLIT[:k]) // whole for k in range(len(SPLIT) + 1)]
    return minor, n_row // minor, n_col // CORES, offs


def ds(start, size, step):
    return pl.ds(pl.multiple_of(start, step), size)


def slot_place(a, major, t):
    near = jnp.minimum(a, major - 1 - a)
    step = (t + 1) // 2
    toward = jnp.where(a > major - 1 - a, step, -step)
    both = a + toward if t % 2 else a - toward
    left = a - (t - near)
    right = a + (t - near)
    one = jnp.where(a > major - 1 - a, left, right)
    return jnp.where(t <= 2 * near, both, one) if t else a


def kernel(
    n_row, n_col, new_hbm, old_hbm, grm_hbm, counts_hbm, affected_hbm,
    res, old_buf, new_buf, gain,
    new_in, old_in, new_code, old_code, part, part_y, part_z, counts, affected,
    load_sem, sum_recv, far, near, x_recv, sib_recv, own_recv, new_recv, sent,
):
    snps = new_in.shape[1]
    new_rows, old_rows = new_in.shape[0], old_in.shape[0]
    out_rows, out_cols = res.shape
    tile = out_cols // counts.shape[0]
    minor, major, chips, offs = sizes_of(n_row, n_col, new_rows, old_rows)
    pieces = len(offs) - 1
    last = pieces - 1
    new_chunk = new_rows // NEW_CHUNKS
    final = NEW_CHUNKS - 1
    group = minor * new_rows
    folds = snps // FOLD
    unit = new_chunk

    row, col = lax.axis_index("row"), lax.axis_index("col")
    a, b = row // minor, row % minor
    chip, core = col // CORES, col % CORES
    sibling = chip * CORES + (CORES - 1 - core)
    has_left, has_right = a > 0, a < major - 1

    def span(k):
        return offs[k + 1] - offs[k]

    grain = min(span(k) for k in range(pieces))

    old_loads = [
        pltpu.make_async_copy(
            old_hbm.at[pl.ds(lo, hi - lo), :], old_in.at[pl.ds(lo, hi - lo), :], load_sem.at[i]
        )
        for i, (lo, hi) in enumerate(((0, offs[1]), (offs[1], old_rows)))
    ]
    new_load = pltpu.make_async_copy(new_hbm, new_in, load_sem.at[2])
    grm_load = pltpu.make_async_copy(grm_hbm, res, load_sem.at[3])
    counts_load = pltpu.make_async_copy(counts_hbm, counts, load_sem.at[4])
    affected_load = pltpu.make_async_copy(affected_hbm, affected, load_sem.at[5])
    old_loads[0].start()
    new_load.start()
    old_loads[1].start()
    counts_load.start()
    affected_load.start()

    barrier = pltpu.get_barrier_semaphore()

    def greet(device):
        pl.semaphore_signal(barrier, inc=1, device_id=device, device_id_type=MESH)

    greet((row, sibling))
    for d in range(1, chips):
        greet((row, (chip + d) % chips * CORES + core))
    for d in range(1, minor):
        greet((a * minor + (b + d) % minor, col))

    @pl.when(has_left)
    def _():
        greet((row - minor, col))

    @pl.when(has_right)
    def _():
        greet((row + minor, col))

    def score_place(j, k):
        return j // CORES * (CORES * old_rows) + CORES * offs[k] + j % CORES * span(k)

    def code_place(j, k):
        return j // CORES * (CORES * offs[CODED]) + CORES * offs[k] + j % CORES * span(k)

    def exact_part(j, k):
        return old_buf.at[ds(score_place(j, k), span(k), grain), :]

    def old_part(j, k):
        if k < CODED:
            return old_code.at[ds(code_place(j, k), span(k), grain), :]
        return exact_part(j, k)

    own_start = col * old_rows

    def own_part(k):
        if k < CODED:
            return old_part(col, k)
        return old_buf.at[ds(own_start + offs[k], span(k), grain), :]

    def new_part(r, k):
        return new_code.at[ds(r * new_rows + k * new_chunk, new_chunk, new_chunk), :]

    def far_copy(k, d):
        return pltpu.make_async_remote_copy(
            own_part(k), old_part(col, k), sent.at[0], x_recv.at[chips - d - 1, k],
            device_id=(row, (chip + d) % chips * CORES + core), device_id_type=MESH,
        )

    def far_taken(k, d):
        j = (chip + d) % chips * CORES + core
        return pltpu.make_async_remote_copy(
            old_part(j, k), old_part(j, k), sent.at[0], x_recv.at[d - 1, k],
            device_id=(row, j), device_id_type=MESH,
        )

    def pass_copy(k, d, which):
        j = (chip + d) % chips * CORES + which
        return pltpu.make_async_remote_copy(
            old_part(j, k), old_part(j, k), sent.at[0], sib_recv.at[d - 1, k],
            device_id=(row, sibling), device_id_type=MESH,
        )

    def own_copy(j):
        part_of = old_buf.at[ds(j * old_rows, old_rows, grain), :]
        return pltpu.make_async_remote_copy(
            part_of, part_of, sent.at[0], own_recv.at[0],
            device_id=(row, sibling), device_id_type=MESH,
        )

    def new_copy(r, k, to):
        return pltpu.make_async_remote_copy(
            new_part(r, k), new_part(r, k), sent.at[0], new_recv.at[r, k],
            device_id=(to, col), device_id_type=MESH,
        )

    sends = []

    def start(copy, cond=None):
        if cond is None:
            copy.start()
        else:
            @pl.when(cond)
            def _():
                copy.start()
        sends.append((cond, copy))

    def is_end(z):
        return (z == 0) | (z == major - 1)

    def encode(x):
        return ((x * LEVELS + 0.5).astype(jnp.int32) - LEVELS).astype(jnp.int16)

    def encode_old(k):
        old_code[ds(code_place(col, k), span(k), grain), :] = encode(
            old_in[offs[k]:offs[k + 1], :]
        )

    def send_sums(buf, me, count, recv, target):
        for d in range(1, count):
            copy = pltpu.make_async_remote_copy(
                buf.at[me], buf.at[me], sent.at[0], recv,
                device_id=target((me + d) % count), device_id_type=MESH,
            )
            start(copy)

    def take_sums(buf, me, count, recv, target):
        rest = buf.at[pl.ds(0, count - 1)]
        pltpu.make_async_copy(rest, rest, recv).wait()
        total = buf[0]
        for i in range(1, count):
            total = total + buf[i]
        return total

    over_col = (part, col, n_col, sum_recv.at[0], lambda i: (row, i))
    over_mid = (part_y, b, minor, sum_recv.at[1], lambda i: (a * minor + i, col))
    over_row = (part_z, a, major, sum_recv.at[2], lambda i: (i * minor + b, col))

    def far_tell(h):
        @pl.when(has_right & (a - (h - 1) >= 0))
        def _():
            pl.semaphore_signal(
                far.at[h - 2], inc=1, device_id=(row + minor, col), device_id_type=MESH
            )

        @pl.when(has_left & (a + (h - 1) <= major - 1))
        def _():
            pl.semaphore_signal(
                far.at[h - 2], inc=1, device_id=(row - minor, col), device_id_type=MESH
            )

    def far_hear(h):
        heard = (a - h >= 0).astype(jnp.int32) + (a + h <= major - 1).astype(jnp.int32)

        @pl.when(heard > 0)
        def _():
            pl.semaphore_wait(far.at[h - 2], heard)

    def send_z(k):
        start(new_copy(row, k, row + minor), has_right)
        start(new_copy(row, k, row - minor), has_left)

    def send_y(z, k, cond=None):
        for d in range(1, minor):
            start(new_copy(z * minor + b, k, a * minor + (b + d) % minor), cond)

    lender = core == CORES - 1
    taker = core != CORES - 1

    def send_old(k):
        for d in range(1, chips):
            start(far_copy(k, d), lender if k == last else None)

    def lend(d, which):
        j = (chip + d) % chips * CORES + which
        return pltpu.make_async_remote_copy(
            exact_part(j, last), exact_part(j, last), sent.at[0], x_recv.at[d - 1, pieces],
            device_id=(row, j), device_id_type=MESH,
        )

    def send_lent():
        for d in range(1, chips):
            copy = pltpu.make_async_remote_copy(
                old_buf.at[ds(sibling * old_rows + offs[last], span(last), grain), :],
                exact_part(sibling, last), sent.at[0], x_recv.at[chips - d - 1, pieces],
                device_id=(row, (chip + d) % chips * CORES + core), device_id_type=MESH,
            )
            start(copy, lender)

    def pass_lent(d, which):
        j = (chip + d) % chips * CORES + which
        return pltpu.make_async_remote_copy(
            exact_part(j, last), exact_part(j, last), sent.at[0], sib_recv.at[d - 1, pieces],
            device_id=(row, sibling), device_id_type=MESH,
        )

    with jax.named_scope("load0"):
        old_loads[0].wait()
        encode_old(0)
        new_load.wait()
        new_code[ds(row * new_rows, new_rows, new_rows), :] = encode(new_in[...])
    with jax.named_scope("barrier"):
        pl.semaphore_wait(
            barrier,
            chips + minor - 1 + has_left.astype(jnp.int32) + has_right.astype(jnp.int32),
        )
    send_old(0)
    send_z(0)
    send_y(a, final, lender)
    far_tell(2)
    pl.semaphore_signal(near.at[0], inc=1, device_id=(row, sibling), device_id_type=MESH)
    with jax.named_scope("loadold"):
        old_loads[1].wait()
        mine = jnp.sum(old_in[...], axis=0, keepdims=True)
        for f in range(folds):
            part_y[pl.ds(b, 1), f, :] = mine[:, f * FOLD:(f + 1) * FOLD]
        send_sums(*over_mid)
    with jax.named_scope("first"):
        send_y(a, final, taker)
        for k in reversed(range(final)):
            send_y(a, k)
        for k in range(1, CODED):
            encode_old(k)
        for k in range(1, AHEAD):
            send_old(k)
        grm_load.start()
    with jax.named_scope("hear"):
        for h in range(2, major):
            far_hear(h)
            if h + 1 < major:
                far_tell(h + 1)
    with jax.named_scope("sumy"):
        part_z[a] = take_sums(*over_mid)
        send_sums(*over_row)
        for k in range(1, NEW_CHUNKS):
            send_z(k)

    def sided(s):
        for left in (True, False):
            z = a - 1 - s if left else a + 1 + s
            valid = z >= 0 if left else z < major
            onward = valid & (has_right if left else has_left)
            dest = row + minor if left else row - minor
            yield z, valid, onward, dest

    def relay(s, k):
        for z, valid, onward, dest in sided(s):
            r = z * minor + b

            @pl.when(valid)
            def _():
                new_copy(r, k, row).wait_recv()
            start(new_copy(r, k, dest), onward)
            across = valid & jnp.logical_not(is_end(z)) if k == final else valid
            send_y(z, k, across)

    def relay_first(s):
        for z, valid, onward, dest in sided(s):
            for d in range(1, minor):
                r = z * minor + (b + d) % minor

                @pl.when(valid & is_end(z))
                def _():
                    new_copy(r, final, row).wait_recv()
                start(new_copy(r, final, dest), onward & is_end(z))

    def own_first():
        for d in range(1, minor):
            r = a * minor + (b + d) % minor

            @pl.when(is_end(a))
            def _():
                new_copy(r, final, row).wait_recv()
            start(new_copy(r, final, row + minor), a == 0)
            start(new_copy(r, final, row - minor), a == major - 1)

    def wait_y(t, first=0, stop=NEW_CHUNKS):
        z = slot_place(a, major, t)
        for k in range(first, stop):
            for d in range(1, minor):
                r = z * minor + (b + d) % minor
                copy = new_copy(r, k, row)
                if k < final:
                    copy.wait_recv()
                else:
                    @pl.when(jnp.logical_not(is_end(z)))
                    def _():
                        copy.wait_recv()

    def forward_old(k):
        for d in range(1, chips):
            if k < last:
                far_taken(k, d).wait_recv()
                start(pass_copy(k, d, core))
            else:
                @pl.when(lender)
                def _():
                    far_taken(k, d).wait_recv()
                start(pass_copy(k, d, core), lender)

                @pl.when(lender)
                def _():
                    lend(d, CORES - 1 - core).wait_recv()
                start(pass_lent(d, CORES - 1 - core), lender)

    def wait_sib_own():
        own_copy(sibling).wait_recv()

    def wait_sib_forwarded(k):
        for d in range(1, chips):
            if k < last:
                pass_copy(k, d, CORES - 1 - core).wait_recv()
            else:
                @pl.when(taker)
                def _():
                    pass_copy(k, d, CORES - 1 - core).wait_recv()
                    pass_lent(d, core).wait_recv()

    def add(rows, z, product, row_tile):
        cols = ds(z * group, group, group)
        mark = affected[(z * group) // tile, row_tile].astype(jnp.float32)
        res[rows, cols] = (
            res[rows, cols].astype(jnp.float32) + product * (mark / snps)
        ).astype(jnp.bfloat16)

    def product_of(first, height, step, t0, tn):
        return lax.dot_general(
            old_buf[ds(first, height, step), :], new_buf[t0 * group:(t0 + tn) * group, :],
            (((1,), (1,)), ((), ())), preferred_element_type=jnp.float32,
        )

    def block(where, k0, k1, t0, tn):
        low = CORES * offs[k0]
        height = CORES * (offs[k1] - offs[k0])
        product = product_of(where * CORES * old_rows + low, height, grain, t0, tn)
        for i in range(tn):
            z = slot_place(a, major, t0 + i)
            for k in range(k0, k1):
                for c in range(CORES):
                    first = (where * CORES + c) * old_rows + offs[k]
                    at = CORES * offs[k] - low + c * span(k)
                    add(
                        ds(first, span(k), grain), z,
                        product[at:at + span(k), i * group:(i + 1) * group], first // tile,
                    )

    def local_rows(t0, tn):
        step = min(tile, CORES * old_rows)

        @pl.loop(0, CORES * old_rows // step)
        def _(i):
            first = chip * CORES * old_rows + i * step
            product = product_of(first, step, step, t0, tn)
            for j in range(tn):
                add(
                    ds(first, step, step), slot_place(a, major, t0 + j),
                    product[:, j * group:(j + 1) * group], first // tile,
                )

    def far_rows(k0, k1, t0, tn):
        for d in range(1, chips):
            block((chip + d) % chips, k0, k1, t0, tn)

    with jax.named_scope("relay0"):
        relay(0, 0)
    with jax.named_scope("own_first"):
        own_first()
    with jax.named_scope("sumz"):
        part[col] = take_sums(*over_row)
        pl.semaphore_wait(near.at[0], 1)
        send_sums(*over_col)
        for k in range(AHEAD, CODED):
            send_old(k)
    with jax.named_scope("relay1"):
        for k in range(1, NEW_CHUNKS):
            relay(0, k)
    with jax.named_scope("x0"):
        forward_old(0)
    with jax.named_scope("sumcol"):
        total = take_sums(*over_col)
    totals = jnp.concatenate([total[f:f + 1] for f in range(folds)], axis=1)
    doubled = totals / (old_rows * n_row * n_col)
    inverse = 1.0 / jnp.sqrt(doubled * (1.0 - 0.5 * doubled) + 0.1)
    code_scale = inverse / LEVELS
    code_shift = (1.0 - doubled) * inverse

    def score(k):
        old_buf[ds(own_start + offs[k], span(k), grain), :] = (
            (old_in[offs[k]:offs[k + 1], :] - doubled) * inverse
        ).astype(jnp.bfloat16)

    with jax.named_scope("score"):
        for k in range(CODED, pieces):
            score(k)
            send_old(k)
        for k in range(CODED):
            score(k)
        start(own_copy(col))
        counts_load.wait()
        affected_load.wait()
        grm_load.wait()

    def decode(codes):
        return codes.astype(jnp.int32).astype(jnp.float32) * code_scale + code_shift

    def decode_new(t, lead=0, rows=None):
        z = slot_place(a, major, t)
        count = counts[(z * group) // tile]

        @pl.loop(0, (rows or group) // STRIP)
        def _(i):
            at = z * group + lead + i * STRIP
            place = lax.broadcasted_iota(jnp.int32, (STRIP, 1), 0) + at % tile
            usable = (place < count).astype(jnp.float32)
            codes = new_code[ds(at, STRIP, STRIP), :]
            new_buf[ds(t * group + lead + i * STRIP, STRIP, STRIP), :] = (
                decode(codes) * usable
            ).astype(jnp.bfloat16)

    def decode_old(k):
        if k >= CODED:
            return
        strip = min(STRIP, CORES * span(k))
        for d in range(1, chips):
            j = (chip + d) % chips * CORES

            @pl.loop(0, CORES * span(k) // strip)
            def _(i):
                codes = old_code[ds(code_place(j, k) + i * strip, strip, strip), :]
                old_buf[ds(score_place(j, k) + i * strip, strip, strip), :] = (
                    decode(codes).astype(jnp.bfloat16)
                )

    def take_group(t):
        with jax.named_scope("wy%d" % t):
            wait_y(t)
        with jax.named_scope("dec%d" % t):
            decode_new(t)

    def take_old(k):
        with jax.named_scope("ws%d" % k):
            wait_sib_forwarded(k)
            decode_old(k)

    with jax.named_scope("gain"):
        for i in range(out_rows // tile):
            for j in range(out_cols // tile):
                mark = affected[j, i].astype(jnp.float32)
                gain[i:i + 1, j * tile:(j + 1) * tile] = jnp.full(
                    (1, tile), mark / snps, jnp.float32
                )

    def relayed(s, k):
        with jax.named_scope("relay%d_%d" % (s, k)):
            relay(s, k)

    def relayed_first(s):
        with jax.named_scope("first%d" % s):
            relay_first(s)

    def forwarded(k):
        with jax.named_scope("x%d" % k):
            forward_old(k)

    def local(t0, tn):
        with jax.named_scope("mm_local%d" % t0):
            local_rows(t0, tn)

    def distant(k0, k1, t0, tn):
        with jax.named_scope("mm_far%d_%d" % (k0, t0)):
            far_rows(k0, k1, t0, tn)

    forwarded(1)
    take_group(0)
    take_old(0)
    relayed(1, 0)
    relayed_first(0)
    with jax.named_scope("sibown"):
        wait_sib_own()
        send_lent()
    local(0, 1)
    take_old(1)
    relayed(1, 1)
    distant(0, 2, 0, 1)
    take_group(1)
    local(1, 1)
    distant(0, 2, 1, 1)
    for s in range(2, major - 1):
        relayed(s, 0)
        relayed_first(s - 1)
        if s == 2:
            forwarded(2)
            take_old(2)
            distant(2, 3, 0, 2)
        relayed(s, 1)
    for t in range(2, major - 1):
        take_group(t)
        local(t, 1)
        distant(0, LATE, t, 1)
    forwarded(3)
    with jax.named_scope("early"):
        decode_new(major - 1, b * new_rows, new_rows)
        wait_y(major - 1, 0, final)
        for d in range(1, minor):
            decode_new(major - 1, (b + d) % minor * new_rows, final * new_chunk)
    relayed_first(major - 2)
    with jax.named_scope("rest"):
        wait_y(major - 1, final)
        for d in range(1, minor):
            decode_new(major - 1, (b + d) % minor * new_rows + final * new_chunk, new_chunk)
    local(major - 1, 1)
    forwarded(4)
    distant(0, LATE, major - 1, 1)
    for k in range(LATE, pieces):
        take_old(k)

    with jax.named_scope("sends"):
        for cond, copy in sends:
            if cond is None:
                copy.wait_send()
            else:
                @pl.when(cond)
                def _():
                    copy.wait_send()


def finish(n_row, n_col, res, old_buf, new_buf, gain, out_hbm, stage, sem):
    out_rows, out_cols = res.shape
    old_rows, new_rows = out_rows // n_col, out_cols // n_row
    minor, major, chips, offs = sizes_of(n_row, n_col, new_rows, old_rows)
    group = minor * new_rows
    tile = out_rows // gain.shape[0]
    early, size = offs[LATE], old_rows - offs[LATE]
    grain = min(hi - lo for lo, hi in zip(offs[:-1], offs[1:], strict=True))
    row, col = lax.axis_index("row"), lax.axis_index("col")
    a, chip = row // minor, col // CORES

    def out_copy(src, start, count):
        return pltpu.make_async_copy(
            src, out_hbm.at[ds(start, count, grain), :], sem.at[0]
        )

    mine = chip * CORES * old_rows
    copies = [
        out_copy(res.at[ds(mine, CORES * old_rows, grain), :], mine, CORES * old_rows)
    ]
    for d in range(1, chips):
        for c in range(CORES):
            first = ((chip + d) % chips * CORES + c) * old_rows
            copies.append(out_copy(res.at[ds(first, early, grain), :], first, early))
    for copy in copies:
        copy.start()
    tails = []
    for d in range(1, chips):
        for c in range(CORES):
            to = ((d - 1) * CORES + c) * size
            start_row = ((chip + d) % chips * CORES + c) * old_rows + early
            tails.append(out_copy(stage.at[pl.ds(to, size), :], start_row, size))

    @pl.when(row >= 0)
    def _():
        for d in range(1, chips):
            where = (chip + d) % chips
            low = where * CORES * old_rows + CORES * early
            product = lax.dot_general(
                old_buf[ds(low, CORES * size, grain), :], new_buf[...],
                (((1,), (1,)), ((), ())), preferred_element_type=jnp.float32,
            )
            for c in range(CORES):
                to = ((d - 1) * CORES + c) * size
                for k in range(LATE, len(offs) - 1):
                    span = offs[k + 1] - offs[k]
                    lead = offs[k] - early
                    at = CORES * lead + c * span
                    first = (where * CORES + c) * old_rows + offs[k]
                    for t in range(major):
                        cols = ds(slot_place(a, major, t) * group, group, group)
                        stage[to + lead:to + lead + span, cols] = (
                            res[ds(first, span, grain), cols].astype(jnp.float32)
                            + product[at:at + span, t * group:(t + 1) * group]
                            * gain[pl.ds(first // tile, 1), cols]
                        ).astype(jnp.bfloat16)
                tails[(d - 1) * CORES + c].start()

    with jax.named_scope("out"):
        for copy in copies + tails:
            copy.wait()


def on_device(new_dosage, old_dosage, grm, counts, affected):
    n_row, n_col = lax.axis_size("row"), lax.axis_size("col")
    new_rows, snps = new_dosage.shape
    old_rows = old_dosage.shape[0]
    out_rows, out_cols = grm.shape
    minor, major, chips, offs = sizes_of(n_row, n_col, new_rows, old_rows)
    pieces = len(offs) - 1
    dma = pltpu.SemaphoreType.DMA
    hbm = pl.BlockSpec(memory_space=pltpu.HBM)
    vmem = pl.BlockSpec(memory_space=pltpu.VMEM)
    row_tiles = affected.shape[0]
    res, old_buf, new_buf, gain = pl.pallas_call(
        functools.partial(kernel, n_row, n_col),
        out_shape=(
            pltpu.VMEM(grm.shape, grm.dtype),
            pltpu.VMEM((old_rows * n_col, snps), jnp.bfloat16),
            pltpu.VMEM((new_rows * n_row, snps), jnp.bfloat16),
            pltpu.VMEM((row_tiles, out_cols), jnp.float32),
        ),
        in_specs=[hbm] * 5,
        out_specs=(vmem,) * 4,
        scratch_shapes=[
            pltpu.VMEM((new_rows, snps), jnp.float32),
            pltpu.VMEM((old_rows, snps), jnp.float32),
            pltpu.VMEM((new_rows * n_row, snps), jnp.int16),
            pltpu.VMEM((offs[CODED] * n_col, snps), jnp.int16),
            pltpu.VMEM((n_col, snps // FOLD, FOLD), jnp.float32),
            pltpu.VMEM((minor, snps // FOLD, FOLD), jnp.float32),
            pltpu.VMEM((major, snps // FOLD, FOLD), jnp.float32),
            pltpu.SMEM(counts.shape, jnp.int32),
            pltpu.SMEM(affected.shape[::-1], jnp.int32),
            dma((6,)),
            dma((3,)),
            pltpu.SemaphoreType.REGULAR((max(1, major - 2),)),
            pltpu.SemaphoreType.REGULAR((1,)),
            dma((chips - 1, pieces + 1)),
            dma((chips - 1, pieces + 1)),
            dma((1,)),
            dma((n_row, NEW_CHUNKS)),
            dma((1,)),
        ],
        compiler_params=pltpu.CompilerParams(
            collective_id=0, has_side_effects=True, vmem_limit_bytes=50 * 1024 * 1024
        ),
    )(new_dosage, old_dosage, grm, counts, affected.T)
    size = old_rows - offs[LATE]
    return pl.pallas_call(
        functools.partial(finish, n_row, n_col),
        out_shape=jax.ShapeDtypeStruct(grm.shape, grm.dtype),
        in_specs=[vmem] * 4,
        out_specs=hbm,
        scratch_shapes=[
            pltpu.VMEM(((chips - 1) * CORES * size, out_cols), jnp.bfloat16),
            dma((1,)),
        ],
        compiler_params=pltpu.CompilerParams(vmem_limit_bytes=12 * 1024 * 1024),
    )(res, old_buf, new_buf, gain)


def solution(mesh):
    return jax.shard_map(
        on_device,
        mesh=mesh,
        in_specs=(
            P(("col", "row"), None),
            P(("row", "col"), None),
            P("row", "col"),
            P("col"),
            P("row", "col"),
        ),
        out_specs=P("row", "col"),
        check_vma=False,
    )
```

```python
import functools

import jax
import jax.numpy as jnp
from jax import lax
from jax.experimental import pallas as pl
from jax.experimental.pallas import tpu as pltpu
from jax.sharding import PartitionSpec as P

MESH = pl.DeviceIdType.MESH
CORES = 2
SPLIT = (4, 2, 4, 4, 2)
AHEAD = 2
CODED = 3
LATE = 3
NEW_CHUNKS = 2
FOLD = 128
LEVELS = 32767
STRIP = 32


def sizes_of(n_row, n_col, new_rows, old_rows):
    minor = 1 << ((n_row.bit_length() - 1) // 2)
    whole = sum(SPLIT)
    offs = [old_rows * sum(SPLIT[:k]) // whole for k in range(len(SPLIT) + 1)]
    return minor, n_row // minor, n_col // CORES, offs


def ds(start, size, step):
    return pl.ds(pl.multiple_of(start, step), size)


def slot_place(a, major, t):
    near = jnp.minimum(a, major - 1 - a)
    step = (t + 1) // 2
    toward = jnp.where(a > major - 1 - a, step, -step)
    both = a + toward if t % 2 else a - toward
    left = a - (t - near)
    right = a + (t - near)
    one = jnp.where(a > major - 1 - a, left, right)
    return jnp.where(t <= 2 * near, both, one) if t else a


def kernel(
    n_row, n_col, new_hbm, old_hbm, grm_hbm, counts_hbm, affected_hbm,
    res, old_buf, new_buf, gain,
    new_in, old_in, new_code, old_code, part, part_y, part_z, counts, affected,
    load_sem, sum_recv, far, x_recv, sib_recv, own_recv, new_recv, sent,
):
    snps = new_in.shape[1]
    new_rows, old_rows = new_in.shape[0], old_in.shape[0]
    out_rows, out_cols = res.shape
    tile = out_cols // counts.shape[0]
    minor, major, chips, offs = sizes_of(n_row, n_col, new_rows, old_rows)
    pieces = len(offs) - 1
    last = pieces - 1
    new_chunk = new_rows // NEW_CHUNKS
    final = NEW_CHUNKS - 1
    group = minor * new_rows
    folds = snps // FOLD
    unit = new_chunk

    row, col = lax.axis_index("row"), lax.axis_index("col")
    a, b = row // minor, row % minor
    chip, core = col // CORES, col % CORES
    sibling = chip * CORES + (CORES - 1 - core)
    has_left, has_right = a > 0, a < major - 1

    def span(k):
        return offs[k + 1] - offs[k]

    grain = min(span(k) for k in range(pieces))

    old_loads = [
        pltpu.make_async_copy(
            old_hbm.at[pl.ds(lo, hi - lo), :], old_in.at[pl.ds(lo, hi - lo), :], load_sem.at[i]
        )
        for i, (lo, hi) in enumerate(((0, offs[1]), (offs[1], old_rows)))
    ]
    new_load = pltpu.make_async_copy(new_hbm, new_in, load_sem.at[2])
    grm_load = pltpu.make_async_copy(grm_hbm, res, load_sem.at[3])
    counts_load = pltpu.make_async_copy(counts_hbm, counts, load_sem.at[4])
    affected_load = pltpu.make_async_copy(affected_hbm, affected, load_sem.at[5])
    old_loads[0].start()
    new_load.start()
    old_loads[1].start()
    counts_load.start()
    affected_load.start()

    barrier = pltpu.get_barrier_semaphore()

    def greet(device):
        pl.semaphore_signal(barrier, inc=1, device_id=device, device_id_type=MESH)

    for d in range(1, n_col):
        greet((row, (col + d) % n_col))
    for d in range(1, minor):
        greet((a * minor + (b + d) % minor, col))

    @pl.when(has_left)
    def _():
        greet((row - minor, col))

    @pl.when(has_right)
    def _():
        greet((row + minor, col))

    def score_place(j, k):
        return j // CORES * (CORES * old_rows) + CORES * offs[k] + j % CORES * span(k)

    def code_place(j, k):
        return j // CORES * (CORES * offs[CODED]) + CORES * offs[k] + j % CORES * span(k)

    def exact_part(j, k):
        return old_buf.at[ds(score_place(j, k), span(k), grain), :]

    def old_part(j, k):
        if k < CODED:
            return old_code.at[ds(code_place(j, k), span(k), grain), :]
        return exact_part(j, k)

    own_start = col * old_rows

    def own_part(k):
        if k < CODED:
            return old_part(col, k)
        return old_buf.at[ds(own_start + offs[k], span(k), grain), :]

    def new_part(r, k):
        return new_code.at[ds(r * new_rows + k * new_chunk, new_chunk, new_chunk), :]

    def far_copy(k, d):
        return pltpu.make_async_remote_copy(
            own_part(k), old_part(col, k), sent.at[0], x_recv.at[chips - d - 1, k],
            device_id=(row, (chip + d) % chips * CORES + core), device_id_type=MESH,
        )

    def far_taken(k, d):
        j = (chip + d) % chips * CORES + core
        return pltpu.make_async_remote_copy(
            old_part(j, k), old_part(j, k), sent.at[0], x_recv.at[d - 1, k],
            device_id=(row, j), device_id_type=MESH,
        )

    def pass_copy(k, d, which):
        j = (chip + d) % chips * CORES + which
        return pltpu.make_async_remote_copy(
            old_part(j, k), old_part(j, k), sent.at[0], sib_recv.at[d - 1, k],
            device_id=(row, sibling), device_id_type=MESH,
        )

    def own_copy(j):
        part_of = old_buf.at[ds(j * old_rows, old_rows, grain), :]
        return pltpu.make_async_remote_copy(
            part_of, part_of, sent.at[0], own_recv.at[0],
            device_id=(row, sibling), device_id_type=MESH,
        )

    def new_copy(r, k, to):
        return pltpu.make_async_remote_copy(
            new_part(r, k), new_part(r, k), sent.at[0], new_recv.at[r, k],
            device_id=(to, col), device_id_type=MESH,
        )

    sends = []

    def start(copy, cond=None):
        if cond is None:
            copy.start()
        else:
            @pl.when(cond)
            def _():
                copy.start()
        sends.append((cond, copy))

    def is_end(z):
        return (z == 0) | (z == major - 1)

    def encode(x):
        return ((x * LEVELS + 0.5).astype(jnp.int32) - LEVELS).astype(jnp.int16)

    def encode_old(k):
        old_code[ds(code_place(col, k), span(k), grain), :] = encode(
            old_in[offs[k]:offs[k + 1], :]
        )

    def send_sums(buf, me, count, recv, target):
        for d in range(1, count):
            copy = pltpu.make_async_remote_copy(
                buf.at[me], buf.at[me], sent.at[0], recv,
                device_id=target((me + d) % count), device_id_type=MESH,
            )
            start(copy)

    def take_sums(buf, me, count, recv, target):
        rest = buf.at[pl.ds(0, count - 1)]
        pltpu.make_async_copy(rest, rest, recv).wait()
        total = buf[0]
        for i in range(1, count):
            total = total + buf[i]
        return total

    over_col = (part, col, n_col, sum_recv.at[0], lambda i: (row, i))
    over_mid = (part_y, b, minor, sum_recv.at[1], lambda i: (a * minor + i, col))
    over_row = (part_z, a, major, sum_recv.at[2], lambda i: (i * minor + b, col))

    def far_tell(h):
        @pl.when(has_right & (a - (h - 1) >= 0))
        def _():
            pl.semaphore_signal(
                far.at[h - 2], inc=1, device_id=(row + minor, col), device_id_type=MESH
            )

        @pl.when(has_left & (a + (h - 1) <= major - 1))
        def _():
            pl.semaphore_signal(
                far.at[h - 2], inc=1, device_id=(row - minor, col), device_id_type=MESH
            )

    def far_hear(h):
        heard = (a - h >= 0).astype(jnp.int32) + (a + h <= major - 1).astype(jnp.int32)

        @pl.when(heard > 0)
        def _():
            pl.semaphore_wait(far.at[h - 2], heard)

    def send_z(k):
        start(new_copy(row, k, row + minor), has_right)
        start(new_copy(row, k, row - minor), has_left)

    def send_y(z, k, cond=None):
        for d in range(1, minor):
            start(new_copy(z * minor + b, k, a * minor + (b + d) % minor), cond)

    lender = core == CORES - 1
    taker = core != CORES - 1

    def send_old(k):
        for d in range(1, chips):
            start(far_copy(k, d), lender if k == last else None)

    def lend(d, which):
        j = (chip + d) % chips * CORES + which
        return pltpu.make_async_remote_copy(
            exact_part(j, last), exact_part(j, last), sent.at[0], x_recv.at[d - 1, pieces],
            device_id=(row, j), device_id_type=MESH,
        )

    def send_lent():
        for d in range(1, chips):
            copy = pltpu.make_async_remote_copy(
                old_buf.at[ds(sibling * old_rows + offs[last], span(last), grain), :],
                exact_part(sibling, last), sent.at[0], x_recv.at[chips - d - 1, pieces],
                device_id=(row, (chip + d) % chips * CORES + core), device_id_type=MESH,
            )
            start(copy, lender)

    def pass_lent(d, which):
        j = (chip + d) % chips * CORES + which
        return pltpu.make_async_remote_copy(
            exact_part(j, last), exact_part(j, last), sent.at[0], sib_recv.at[d - 1, pieces],
            device_id=(row, sibling), device_id_type=MESH,
        )

    with jax.named_scope("load0"):
        old_loads[0].wait()
        encode_old(0)
        new_load.wait()
        new_code[ds(row * new_rows, new_rows, new_rows), :] = encode(new_in[...])
    with jax.named_scope("barrier"):
        pl.semaphore_wait(
            barrier,
            n_col - 1 + minor - 1 + has_left.astype(jnp.int32) + has_right.astype(jnp.int32),
        )
    send_old(0)
    send_z(0)
    far_tell(2)
    with jax.named_scope("loadold"):
        old_loads[1].wait()
        mine = jnp.sum(old_in[...], axis=0, keepdims=True)
        for f in range(folds):
            part_y[pl.ds(b, 1), f, :] = mine[:, f * FOLD:(f + 1) * FOLD]
        send_sums(*over_mid)
    with jax.named_scope("first"):
        for k in reversed(range(NEW_CHUNKS)):
            send_y(a, k)
        for k in range(1, CODED):
            encode_old(k)
        for k in range(1, AHEAD):
            send_old(k)
        grm_load.start()
    with jax.named_scope("hear"):
        for h in range(2, major):
            far_hear(h)
            if h + 1 < major:
                far_tell(h + 1)
    with jax.named_scope("sumy"):
        part_z[a] = take_sums(*over_mid)
        send_sums(*over_row)
        for k in range(1, NEW_CHUNKS):
            send_z(k)

    def sided(s):
        for left in (True, False):
            z = a - 1 - s if left else a + 1 + s
            valid = z >= 0 if left else z < major
            onward = valid & (has_right if left else has_left)
            dest = row + minor if left else row - minor
            yield z, valid, onward, dest

    def relay(s, k):
        for z, valid, onward, dest in sided(s):
            r = z * minor + b

            @pl.when(valid)
            def _():
                new_copy(r, k, row).wait_recv()
            start(new_copy(r, k, dest), onward)
            across = valid & jnp.logical_not(is_end(z)) if k == final else valid
            send_y(z, k, across)

    def relay_first(s):
        for z, valid, onward, dest in sided(s):
            for d in range(1, minor):
                r = z * minor + (b + d) % minor

                @pl.when(valid & is_end(z))
                def _():
                    new_copy(r, final, row).wait_recv()
                start(new_copy(r, final, dest), onward & is_end(z))

    def own_first():
        for d in range(1, minor):
            r = a * minor + (b + d) % minor

            @pl.when(is_end(a))
            def _():
                new_copy(r, final, row).wait_recv()
            start(new_copy(r, final, row + minor), a == 0)
            start(new_copy(r, final, row - minor), a == major - 1)

    def wait_y(t, first=0, stop=NEW_CHUNKS):
        z = slot_place(a, major, t)
        for k in range(first, stop):
            for d in range(1, minor):
                r = z * minor + (b + d) % minor
                copy = new_copy(r, k, row)
                if k < final:
                    copy.wait_recv()
                else:
                    @pl.when(jnp.logical_not(is_end(z)))
                    def _():
                        copy.wait_recv()

    def forward_old(k):
        for d in range(1, chips):
            if k < last:
                far_taken(k, d).wait_recv()
                start(pass_copy(k, d, core))
            else:
                @pl.when(lender)
                def _():
                    far_taken(k, d).wait_recv()
                start(pass_copy(k, d, core), lender)

                @pl.when(lender)
                def _():
                    lend(d, CORES - 1 - core).wait_recv()
                start(pass_lent(d, CORES - 1 - core), lender)

    def wait_sib_own():
        own_copy(sibling).wait_recv()

    def wait_sib_forwarded(k):
        for d in range(1, chips):
            if k < last:
                pass_copy(k, d, CORES - 1 - core).wait_recv()
            else:
                @pl.when(taker)
                def _():
                    pass_copy(k, d, CORES - 1 - core).wait_recv()
                    pass_lent(d, core).wait_recv()

    def add(rows, z, product, row_tile):
        cols = ds(z * group, group, group)
        mark = affected[(z * group) // tile, row_tile].astype(jnp.float32)
        res[rows, cols] = (
            res[rows, cols].astype(jnp.float32) + product * (mark / snps)
        ).astype(jnp.bfloat16)

    def product_of(first, height, step, t0, tn):
        return lax.dot_general(
            old_buf[ds(first, height, step), :], new_buf[t0 * group:(t0 + tn) * group, :],
            (((1,), (1,)), ((), ())), preferred_element_type=jnp.float32,
        )

    def block(where, k0, k1, t0, tn):
        low = CORES * offs[k0]
        height = CORES * (offs[k1] - offs[k0])
        product = product_of(where * CORES * old_rows + low, height, grain, t0, tn)
        for i in range(tn):
            z = slot_place(a, major, t0 + i)
            for k in range(k0, k1):
                for c in range(CORES):
                    first = (where * CORES + c) * old_rows + offs[k]
                    at = CORES * offs[k] - low + c * span(k)
                    add(
                        ds(first, span(k), grain), z,
                        product[at:at + span(k), i * group:(i + 1) * group], first // tile,
                    )

    def local_rows(t0, tn):
        step = min(tile, CORES * old_rows)

        @pl.loop(0, CORES * old_rows // step)
        def _(i):
            first = chip * CORES * old_rows + i * step
            product = product_of(first, step, step, t0, tn)
            for j in range(tn):
                add(
                    ds(first, step, step), slot_place(a, major, t0 + j),
                    product[:, j * group:(j + 1) * group], first // tile,
                )

    def far_rows(k0, k1, t0, tn):
        for d in range(1, chips):
            block((chip + d) % chips, k0, k1, t0, tn)

    with jax.named_scope("relay0"):
        relay(0, 0)
    with jax.named_scope("own_first"):
        own_first()
    with jax.named_scope("sumz"):
        part[col] = take_sums(*over_row)
        send_sums(*over_col)
        for k in range(AHEAD, CODED):
            send_old(k)
    with jax.named_scope("relay1"):
        for k in range(1, NEW_CHUNKS):
            relay(0, k)
    with jax.named_scope("x0"):
        forward_old(0)
    with jax.named_scope("sumcol"):
        total = take_sums(*over_col)
    totals = jnp.concatenate([total[f:f + 1] for f in range(folds)], axis=1)
    doubled = totals / (old_rows * n_row * n_col)
    inverse = 1.0 / jnp.sqrt(doubled * (1.0 - 0.5 * doubled) + 0.1)
    code_scale = inverse / LEVELS
    code_shift = (1.0 - doubled) * inverse

    def score(k):
        old_buf[ds(own_start + offs[k], span(k), grain), :] = (
            (old_in[offs[k]:offs[k + 1], :] - doubled) * inverse
        ).astype(jnp.bfloat16)

    with jax.named_scope("score"):
        for k in range(CODED, pieces):
            score(k)
            send_old(k)
        for k in range(CODED):
            score(k)
        start(own_copy(col))
        counts_load.wait()
        affected_load.wait()
        grm_load.wait()

    def decode(codes):
        return codes.astype(jnp.int32).astype(jnp.float32) * code_scale + code_shift

    def decode_new(t, lead=0, rows=None):
        z = slot_place(a, major, t)
        count = counts[(z * group) // tile]

        @pl.loop(0, (rows or group) // STRIP)
        def _(i):
            at = z * group + lead + i * STRIP
            place = lax.broadcasted_iota(jnp.int32, (STRIP, 1), 0) + at % tile
            usable = (place < count).astype(jnp.float32)
            codes = new_code[ds(at, STRIP, STRIP), :]
            new_buf[ds(t * group + lead + i * STRIP, STRIP, STRIP), :] = (
                decode(codes) * usable
            ).astype(jnp.bfloat16)

    def decode_old(k):
        if k >= CODED:
            return
        strip = min(STRIP, CORES * span(k))
        for d in range(1, chips):
            j = (chip + d) % chips * CORES

            @pl.loop(0, CORES * span(k) // strip)
            def _(i):
                codes = old_code[ds(code_place(j, k) + i * strip, strip, strip), :]
                old_buf[ds(score_place(j, k) + i * strip, strip, strip), :] = (
                    decode(codes).astype(jnp.bfloat16)
                )

    def take_group(t):
        with jax.named_scope("wy%d" % t):
            wait_y(t)
        with jax.named_scope("dec%d" % t):
            decode_new(t)

    def take_old(k):
        with jax.named_scope("ws%d" % k):
            wait_sib_forwarded(k)
            decode_old(k)

    with jax.named_scope("gain"):
        for i in range(out_rows // tile):
            for j in range(out_cols // tile):
                mark = affected[j, i].astype(jnp.float32)
                gain[i:i + 1, j * tile:(j + 1) * tile] = jnp.full(
                    (1, tile), mark / snps, jnp.float32
                )

    def relayed(s, k):
        with jax.named_scope("relay%d_%d" % (s, k)):
            relay(s, k)

    def relayed_first(s):
        with jax.named_scope("first%d" % s):
            relay_first(s)

    def forwarded(k):
        with jax.named_scope("x%d" % k):
            forward_old(k)

    def local(t0, tn):
        with jax.named_scope("mm_local%d" % t0):
            local_rows(t0, tn)

    def distant(k0, k1, t0, tn):
        with jax.named_scope("mm_far%d_%d" % (k0, t0)):
            far_rows(k0, k1, t0, tn)

    forwarded(1)
    take_group(0)
    take_old(0)
    relayed(1, 0)
    relayed_first(0)
    with jax.named_scope("sibown"):
        wait_sib_own()
        send_lent()
    local(0, 1)
    take_old(1)
    relayed(1, 1)
    distant(0, 2, 0, 1)
    take_group(1)
    local(1, 1)
    distant(0, 2, 1, 1)
    for s in range(2, major - 1):
        relayed(s, 0)
        relayed_first(s - 1)
        if s == 2:
            forwarded(2)
            take_old(2)
            distant(2, 3, 0, 2)
        relayed(s, 1)
    for t in range(2, major - 1):
        take_group(t)
        local(t, 1)
        distant(0, LATE, t, 1)
    forwarded(3)
    with jax.named_scope("early"):
        decode_new(major - 1, b * new_rows, new_rows)
        wait_y(major - 1, 0, final)
        for d in range(1, minor):
            decode_new(major - 1, (b + d) % minor * new_rows, final * new_chunk)
    relayed_first(major - 2)
    with jax.named_scope("rest"):
        wait_y(major - 1, final)
        for d in range(1, minor):
            decode_new(major - 1, (b + d) % minor * new_rows + final * new_chunk, new_chunk)
    local(major - 1, 1)
    forwarded(4)
    distant(0, LATE, major - 1, 1)
    for k in range(LATE, pieces):
        take_old(k)

    with jax.named_scope("sends"):
        for cond, copy in sends:
            if cond is None:
                copy.wait_send()
            else:
                @pl.when(cond)
                def _():
                    copy.wait_send()


def finish(n_row, n_col, res, old_buf, new_buf, gain, out_hbm, stage, sem):
    out_rows, out_cols = res.shape
    old_rows, new_rows = out_rows // n_col, out_cols // n_row
    minor, major, chips, offs = sizes_of(n_row, n_col, new_rows, old_rows)
    group = minor * new_rows
    tile = out_rows // gain.shape[0]
    early, size = offs[LATE], old_rows - offs[LATE]
    grain = min(hi - lo for lo, hi in zip(offs[:-1], offs[1:], strict=True))
    row, col = lax.axis_index("row"), lax.axis_index("col")
    a, chip = row // minor, col // CORES

    def out_copy(src, start, count):
        return pltpu.make_async_copy(
            src, out_hbm.at[ds(start, count, grain), :], sem.at[0]
        )

    mine = chip * CORES * old_rows
    copies = [
        out_copy(res.at[ds(mine, CORES * old_rows, grain), :], mine, CORES * old_rows)
    ]
    for d in range(1, chips):
        for c in range(CORES):
            first = ((chip + d) % chips * CORES + c) * old_rows
            copies.append(out_copy(res.at[ds(first, early, grain), :], first, early))
    for copy in copies:
        copy.start()
    tails = []
    for d in range(1, chips):
        for c in range(CORES):
            to = ((d - 1) * CORES + c) * size
            start_row = ((chip + d) % chips * CORES + c) * old_rows + early
            tails.append(out_copy(stage.at[pl.ds(to, size), :], start_row, size))

    @pl.when(row >= 0)
    def _():
        for d in range(1, chips):
            where = (chip + d) % chips
            low = where * CORES * old_rows + CORES * early
            product = lax.dot_general(
                old_buf[ds(low, CORES * size, grain), :], new_buf[...],
                (((1,), (1,)), ((), ())), preferred_element_type=jnp.float32,
            )
            for c in range(CORES):
                to = ((d - 1) * CORES + c) * size
                for k in range(LATE, len(offs) - 1):
                    span = offs[k + 1] - offs[k]
                    lead = offs[k] - early
                    at = CORES * lead + c * span
                    first = (where * CORES + c) * old_rows + offs[k]
                    for t in range(major):
                        cols = ds(slot_place(a, major, t) * group, group, group)
                        stage[to + lead:to + lead + span, cols] = (
                            res[ds(first, span, grain), cols].astype(jnp.float32)
                            + product[at:at + span, t * group:(t + 1) * group]
                            * gain[pl.ds(first // tile, 1), cols]
                        ).astype(jnp.bfloat16)
                tails[(d - 1) * CORES + c].start()

    with jax.named_scope("out"):
        for copy in copies + tails:
            copy.wait()


def on_device(new_dosage, old_dosage, grm, counts, affected):
    n_row, n_col = lax.axis_size("row"), lax.axis_size("col")
    new_rows, snps = new_dosage.shape
    old_rows = old_dosage.shape[0]
    out_rows, out_cols = grm.shape
    minor, major, chips, offs = sizes_of(n_row, n_col, new_rows, old_rows)
    pieces = len(offs) - 1
    dma = pltpu.SemaphoreType.DMA
    hbm = pl.BlockSpec(memory_space=pltpu.HBM)
    vmem = pl.BlockSpec(memory_space=pltpu.VMEM)
    row_tiles = affected.shape[0]
    res, old_buf, new_buf, gain = pl.pallas_call(
        functools.partial(kernel, n_row, n_col),
        out_shape=(
            pltpu.VMEM(grm.shape, grm.dtype),
            pltpu.VMEM((old_rows * n_col, snps), jnp.bfloat16),
            pltpu.VMEM((new_rows * n_row, snps), jnp.bfloat16),
            pltpu.VMEM((row_tiles, out_cols), jnp.float32),
        ),
        in_specs=[hbm] * 5,
        out_specs=(vmem,) * 4,
        scratch_shapes=[
            pltpu.VMEM((new_rows, snps), jnp.float32),
            pltpu.VMEM((old_rows, snps), jnp.float32),
            pltpu.VMEM((new_rows * n_row, snps), jnp.int16),
            pltpu.VMEM((offs[CODED] * n_col, snps), jnp.int16),
            pltpu.VMEM((n_col, snps // FOLD, FOLD), jnp.float32),
            pltpu.VMEM((minor, snps // FOLD, FOLD), jnp.float32),
            pltpu.VMEM((major, snps // FOLD, FOLD), jnp.float32),
            pltpu.SMEM(counts.shape, jnp.int32),
            pltpu.SMEM(affected.shape[::-1], jnp.int32),
            dma((6,)),
            dma((3,)),
            pltpu.SemaphoreType.REGULAR((max(1, major - 2),)),
            dma((chips - 1, pieces + 1)),
            dma((chips - 1, pieces + 1)),
            dma((1,)),
            dma((n_row, NEW_CHUNKS)),
            dma((1,)),
        ],
        compiler_params=pltpu.CompilerParams(
            collective_id=0, has_side_effects=True, vmem_limit_bytes=50 * 1024 * 1024
        ),
    )(new_dosage, old_dosage, grm, counts, affected.T)
    size = old_rows - offs[LATE]
    return pl.pallas_call(
        functools.partial(finish, n_row, n_col),
        out_shape=jax.ShapeDtypeStruct(grm.shape, grm.dtype),
        in_specs=[vmem] * 4,
        out_specs=hbm,
        scratch_shapes=[
            pltpu.VMEM(((chips - 1) * CORES * size, out_cols), jnp.bfloat16),
            dma((1,)),
        ],
        compiler_params=pltpu.CompilerParams(vmem_limit_bytes=12 * 1024 * 1024),
    )(res, old_buf, new_buf, gain)


def solution(mesh):
    return jax.shard_map(
        on_device,
        mesh=mesh,
        in_specs=(
            P(("col", "row"), None),
            P(("row", "col"), None),
            P("row", "col"),
            P("col"),
            P("row", "col"),
        ),
        out_specs=P("row", "col"),
        check_vma=False,
    )
```
